32 devices in a mesh: grp: 2 (over y), kv: 8 (over z, core), hd: 2 (over x), sub: 1.
Axes of the slice: x: 2, y: 2, z: 4, core: 2. Of those that a mesh axis runs over, the one named last changes fastest.
Arguments:
- queries: bfloat16 [256, 8192], P(('grp', 'kv'), 'hd'), parts along dimension 0, may hold values from -12 to 12
- prompt_of: int32 [256, 1], P('grp'), parts along dimension 0, may hold values from 0 to 1; in each aligned block of 16 rows (0 to 15, 16 to 31, ...) at most 8 rows name the same one
- prompt_len: int32 [4], P('grp'), parts along dimension 0, may hold values from 3072 to 4096
- suffix_len: int32 [256], P(('grp', 'kv')), parts along dimension 0, may hold values from 0 to 512
- page_table: int32 [256, 8], P(('grp', 'kv'), 'sub'), parts along dimension 0, may hold values from 0 to 127, as said below
- prompt_keys: bfloat16 [16384, 1024], P(('grp', 'kv', 'sub'), 'hd'), parts along dimension 0, may hold values from -14 to 14
- shared_prompt_values: bfloat16 [16384, 1024], P(('grp', 'kv', 'sub'), 'hd'), parts along dimension 0, may hold values from -6 to 6
- suffix_pool_keys: bfloat16 [2048, 64, 1024], P(('grp', 'kv', 'sub'), None, 'hd'), parts along dimension 0, may hold values from -14 to 14
- suffix_pool_values: bfloat16 [2048, 64, 1024], P(('grp', 'kv', 'sub'), None, 'hd'), parts along dimension 0, may hold values from -6 to 6
Outputs:
- attended: float32 [256, 8192], P(('grp', 'kv'), 'hd'), parts along dimension 0
The draws below stay inside these ranges and needn't reach their ends.
There are 2 independent parts, one for each index of `grp`. The reference program is written for one: setup_inputs(seed, part) draws one part's arguments, and reference() takes and returns one part's arrays. A program takes and returns all parts, laid end to end along the dimension named above; each array names one. Nothing has to cross between parts.
Inputs may be any that keep to these rules, and one draw needn't show every extreme that they name: `prompt_of`: in each aligned block of 16 rows (the sequences of one index of kv), every prompt is named by exactly 8 rows. `page_table`: for each index k of kv and s of sub, the entries in rows k * 16 to (k + 1) * 16 - 1 and columns s * 8 to (s + 1) * 8 - 1 are a permutation of 0 to 127.
All inputs are finite; a program needn't handle non-finite values.
Results may differ from the reference program's by a relative error of at most 0.0011.
Values may be sent and summed in bfloat16 or wider, within the bound.
A program may use at most 128 MiB of HBM per device.

```python
import math
import jax
import jax.numpy as jnp
import numpy as np
from jax import lax

QUERY_HEADS = 64
KEY_VALUE_HEADS = 8
HEAD_SIZE = 128
SEQ_DEV = 16
CACHE_PER_DEVICE = 1024
SUF_MAX = 512
PAGE_POSITIONS = 64
SEQS = 128
REACH = 1024
PROMPT_TOKENS = 8192
PROMPTS = 2
MOST = 8
PAGES_SEQ = 8
HALF_PAGE_SLOTS = 8
POOL_DEV = 128
POOL_PAGES = 1024
N_KV = 8
N_SUB = 1


def offset_key_rows(key, salt, array_shape):
    sampled_array = 2.5 * jax.random.truncated_normal(jax.random.fold_in(key, salt), -4.8, 4.8, array_shape, jnp.float32)
    return sampled_array


def draw_prompt_keys(key, part):
    return offset_key_rows(key, 17, (PROMPT_TOKENS, KEY_VALUE_HEADS * HEAD_SIZE)).astype(jnp.bfloat16)


def draw_suffix_pool_keys(key, part):
    return offset_key_rows(key, 19, (POOL_PAGES, PAGE_POSITIONS, KEY_VALUE_HEADS * HEAD_SIZE)).astype(jnp.bfloat16)


def draw_queries(key, part):
    sampled_array = jax.random.truncated_normal(jax.random.fold_in(key, 29), -6.0, 6.0, (SEQS, QUERY_HEADS * HEAD_SIZE), jnp.float32)
    return sampled_array.astype(jnp.bfloat16)


def local_order(block_key):
    return jax.random.permutation(block_key, POOL_DEV)


def draw_page_table(key, part):
    block_keys = jax.random.split(jax.random.fold_in(key, 41), N_KV * N_SUB)
    orders = jax.vmap(local_order)(block_keys).astype(jnp.int32)
    orders = orders.reshape(N_KV, N_SUB, SEQ_DEV, HALF_PAGE_SLOTS).transpose(0, 2, 1, 3)
    return orders.reshape(SEQS, PAGES_SEQ).astype(jnp.int32)


def set_ends(entries, stream_key, low, high):
    longest = entries.shape.index(max(entries.shape))
    spots = []
    for shift in (0, 1):
        where = [jax.random.randint(jax.random.fold_in(stream_key, axis), (), 0, length) for axis, length in enumerate(entries.shape)]
        where[longest] = (where[longest] + shift) % entries.shape[longest]
        spots.append(tuple(where))
    return entries.at[spots[0]].set(low).at[spots[1]].set(high)


def level_of(own_key, dims, cuts, low, high):
    def one(dim, shards_of):
        heights = jax.random.uniform(jax.random.fold_in(jax.random.fold_in(own_key, 6), dim), (shards_of,), jnp.float32, low / len(cuts), high / len(cuts))
        return jnp.repeat(jnp.exp(heights), dims[dim] // shards_of).reshape((-1,) + (1,) * (len(dims) - dim - 1))

    loudness = one(*cuts[0])
    for cut in cuts[1:]:
        loudness = loudness * one(*cut)
    return loudness


def deal_out(stream_key, own, number, rows, count, top, limit, slope):
    order = jax.random.permutation(stream_key, count)
    heavy_load, common = portions_of(count, rows * top, limit, slope, True), portions_of(count, rows * top, limit, slope, False)
    places = jnp.arange(count)

    def named(sizes, turn):
        used = int((sizes > 0).sum())
        fixed = max(1, used // 4)
        shifted = fixed + (places - fixed + turn * (used - fixed)) % max(1, count - fixed)
        return jnp.zeros((count,), jnp.int32).at[order[jnp.where(places < fixed, places, shifted)]].set(jnp.asarray(sizes, jnp.int32))

    sizes = jnp.where(number % 4 == 0, named(heavy_load, number // 4), named(common, number - number // 4 - 1))
    mixed = jax.random.permutation(jax.random.fold_in(own, 3), count)
    source_of, taker = mixed[0:count // 2 * 2:2], mixed[1:count // 2 * 2:2]
    room = jnp.minimum(sizes[source_of] - 1, limit - sizes[taker]) // 2
    room = jnp.where((source_of == order[0]) | (taker == order[0]) | (sizes[taker] == 0), 0, jnp.maximum(room, 0))
    shifted = jax.random.randint(jax.random.fold_in(own, 4), (count // 2,), 0, 1 << 20) % (room + 1)
    sizes = sizes.at[source_of].add(-shifted).at[taker].add(shifted)
    items = jnp.searchsorted(jnp.cumsum(sizes), jnp.arange(rows * top), side="right").astype(jnp.int32)
    table = items.reshape(top, rows).T
    table = table[jax.random.permutation(jax.random.fold_in(own, 1), rows)]
    turn = jax.random.randint(jax.random.fold_in(own, 2), (rows, 1), 0, top)
    return jnp.take_along_axis(table, (jnp.arange(top)[None, :] + turn) % top, axis=1)


def portions_of(count, total, most, skew, full):
    loads = [(1 << 20) // math.isqrt(rank ** skew) + 1 for rank in range(1, count + 1)]
    largest = most if full else min(most, max(-(-total // count), total * loads[0] // sum(loads)))
    least = 1 if total - largest >= count - 1 else 0
    given, rest = [largest] + [least] * (count - 1), total - largest - least * (count - 1)
    while rest > 0:
        candidates = [i for i in range(1, count) if given[i] < largest] or [i for i in range(1, count) if given[i] < most]
        mass, left = sum([loads[i] for i in candidates]), rest
        for i in candidates:
            extra = min(most - given[i], max(1, left * loads[i] // mass), rest)
            given[i] = given[i] + extra
            rest = rest - extra
    return np.array(given)


def scatter_about(rng, extent, scale, limit, pieces=(), held_as=jnp.bfloat16):
    array = jax.random.normal(rng, extent, jnp.float32) * scale
    if len(pieces) > 0:
        array = level_of(rng, extent, pieces, -0.22, 0.18) * array
    return jnp.clip(array, min=-limit, max=limit).astype(held_as)


def setup_inputs(seed: int = 0, part: int = 0) -> dict:
    arg_keys = jax.random.split(jax.random.key(seed), 10)
    part_splits = jax.random.split(jax.random.fold_in(arg_keys[9], part), 10)
    queries = draw_queries(jax.random.fold_in(jax.random.fold_in(arg_keys[9], part), 71), part)
    prompt_of_keys = jax.random.split(jax.random.fold_in(part_splits[1], 1), SEQS // SEQ_DEV)
    prompt_of_turns = jax.random.permutation(jax.random.fold_in(part_splits[1], 3), SEQS // SEQ_DEV)
    prompt_of = jax.vmap(lambda own, number: deal_out(jax.random.fold_in(part_splits[1], 2), own, number, SEQ_DEV, PROMPTS, 1, MOST, 2))(prompt_of_keys, prompt_of_turns).reshape((SEQS, 1))
    prompt_len = jax.random.randint(part_splits[2], (PROMPTS,), 3 * REACH, 4 * REACH + 1).astype(jnp.int32)
    suffix_len = set_ends(jax.random.randint(part_splits[3], (SEQS,), 0, SUF_MAX + 1), jax.random.fold_in(part_splits[3], 1), 0, SUF_MAX).astype(jnp.int32)
    page_table = draw_page_table(jax.random.fold_in(jax.random.fold_in(arg_keys[9], part), 71), part)
    prompt_keys = draw_prompt_keys(jax.random.fold_in(jax.random.fold_in(arg_keys[9], part), 71), part)
    shared_prompt_values = scatter_about(part_splits[6], (PROMPT_TOKENS, KEY_VALUE_HEADS * HEAD_SIZE), 1.0, 6.0, ((0, 8), (1, 2)))
    suffix_pool_keys = draw_suffix_pool_keys(jax.random.fold_in(jax.random.fold_in(arg_keys[9], part), 71), part)
    suffix_pool_values = scatter_about(part_splits[8], (POOL_PAGES, PAGE_POSITIONS, KEY_VALUE_HEADS * HEAD_SIZE), 1.0, 6.0, ((0, 8), (2, 2)))
    return {"queries": queries, "prompt_of": prompt_of, "prompt_len": prompt_len, "suffix_len": suffix_len, "page_table": page_table, "prompt_keys": prompt_keys, "shared_prompt_values": shared_prompt_values, "suffix_pool_keys": suffix_pool_keys, "suffix_pool_values": suffix_pool_values}


NEGATIVE = -1e+30

def partial_blocks(query_head_rows, key_blocks, value_blocks, key_mask):
    scores = jnp.einsum('kgd,bckd->bkgc', query_head_rows, key_blocks, precision=lax.Precision.HIGHEST)
    scores = scores * (1.0 / math.sqrt(HEAD_SIZE))
    keeper = key_mask[:, None, None, :]
    scores = jnp.where(keeper, scores, NEGATIVE)
    row_max = lax.optimization_barrier(jnp.max(scores, axis=3, keepdims=True))
    weights = jnp.where(keeper, jnp.exp(scores - row_max), 0.0)
    totals = jnp.maximum(lax.optimization_barrier(jnp.sum(weights, axis=3)), 1.0)
    rounded = lax.optimization_barrier(weights.astype(jnp.bfloat16)).astype(jnp.float32)
    blended = jnp.einsum('bkgc,bckd->bkgd', rounded, value_blocks, precision=lax.Precision.HIGHEST)
    return (blended / totals[..., None], row_max[..., 0] + jnp.log(totals))

def reference(queries, prompt_of, prompt_len, suffix_len, page_table, prompt_keys, shared_prompt_values, suffix_pool_keys, suffix_pool_values):
    query_group_size = QUERY_HEADS // KEY_VALUE_HEADS
    block_count = N_KV * N_SUB
    slice_window = min(4 * N_SUB + 1, block_count)
    starts = (jnp.cumsum(prompt_len) - prompt_len).astype(jnp.int32)

    def one_sequence(page_index_value):
        prompt = prompt_of[page_index_value, 0]
        begin = starts[prompt]
        finish = begin + prompt_len[prompt]
        first_block = jnp.minimum(begin // CACHE_PER_DEVICE, block_count - slice_window).astype(jnp.int32)
        offset = (first_block * CACHE_PER_DEVICE).astype(jnp.int32)
        key_slice_window = lax.dynamic_slice_in_dim(prompt_keys, offset, slice_window * CACHE_PER_DEVICE, 0)
        value_slice_window = lax.dynamic_slice_in_dim(shared_prompt_values, offset, slice_window * CACHE_PER_DEVICE, 0)
        key_slice_window = key_slice_window.astype(jnp.float32).reshape(slice_window, CACHE_PER_DEVICE, KEY_VALUE_HEADS, HEAD_SIZE)
        value_slice_window = value_slice_window.astype(jnp.float32).reshape(slice_window, CACHE_PER_DEVICE, KEY_VALUE_HEADS, HEAD_SIZE)
        position = offset + jnp.arange(slice_window * CACHE_PER_DEVICE, dtype=jnp.int32).reshape(slice_window, CACHE_PER_DEVICE)
        prompt_mask = (position >= begin) & (position < finish)
        query_head_rows = queries[page_index_value].astype(jnp.float32).reshape(KEY_VALUE_HEADS, query_group_size, HEAD_SIZE)
        prompt_out, prompt_lse = partial_blocks(query_head_rows, key_slice_window, value_slice_window, prompt_mask)
        owner = (page_index_value // SEQ_DEV).astype(jnp.int32)
        slot_half = (jnp.arange(PAGES_SEQ, dtype=jnp.int32) // HALF_PAGE_SLOTS).astype(jnp.int32)
        page_list = (owner * N_SUB + slot_half) * POOL_DEV + page_table[page_index_value]
        suffix_page_block = suffix_pool_keys[page_list].astype(jnp.float32).reshape(N_SUB, HALF_PAGE_SLOTS * PAGE_POSITIONS, KEY_VALUE_HEADS, HEAD_SIZE)
        suffix_value_rows = suffix_pool_values[page_list].astype(jnp.float32).reshape(N_SUB, HALF_PAGE_SLOTS * PAGE_POSITIONS, KEY_VALUE_HEADS, HEAD_SIZE)
        suffix_pos = jnp.arange(PAGES_SEQ * PAGE_POSITIONS, dtype=jnp.int32).reshape(N_SUB, HALF_PAGE_SLOTS * PAGE_POSITIONS)
        suffix_mask = suffix_pos < suffix_len[page_index_value]
        suffix_out, suffix_lse = partial_blocks(query_head_rows, suffix_page_block, suffix_value_rows, suffix_mask)
        every_lse = jnp.concatenate([prompt_lse, suffix_lse], axis=0)
        every_out = jnp.concatenate([prompt_out, suffix_out], axis=0)
        joint_max = lax.optimization_barrier(jnp.max(every_lse, axis=0))
        factors = jnp.exp(every_lse - joint_max)
        merged = lax.optimization_barrier(jnp.sum(factors[..., None] * every_out, axis=0)) / lax.optimization_barrier(jnp.sum(factors, axis=0))[..., None]
        return merged.reshape(QUERY_HEADS * HEAD_SIZE)
    result = lax.map(one_sequence, jnp.arange(SEQS, dtype=jnp.int32))
    return result.astype(jnp.float32)
```

```python
import functools
import math

import jax
import jax.numpy as jnp
from jax import lax
from jax.experimental import pallas as pl
from jax.experimental.pallas import tpu as pltpu
from jax.sharding import PartitionSpec as P

HEAD_SIZE = 128


NEGATIVE = -1e30


def joined(value, axis, combine):
    everything = jax.tree.map(lambda part: lax.all_gather(part, axis), value)
    leading = jax.tree.map(lambda part: part[0], everything)

    def hop(k, so_far):
        return combine(so_far, jax.tree.map(lambda part: part[k], everything))

    return lax.fori_loop(1, lax.axis_size(axis), hop, leading)


def attend_block(sent_rows, key_block, value_block, lower_bound, upper_bound, first_position):
    row_count = sent_rows.shape[0]
    key_count = key_block.shape[0]
    kv_local = key_block.shape[1] // HEAD_SIZE
    query_group_size = sent_rows.shape[1] // (HEAD_SIZE * kv_local)
    position = first_position + jnp.arange(key_count, dtype=jnp.int32)
    key_mask = (position[None, :] >= lower_bound[:, None]) & (
        position[None, :] < upper_bound[:, None]
    )
    key_mask = key_mask[:, None, :]
    score_scale = 1.0 / math.sqrt(HEAD_SIZE)
    blended_parts = []
    lse_parts = []
    for kv_head in range(kv_local):
        low_column = kv_head * query_group_size * HEAD_SIZE
        head_query = sent_rows[:, low_column : low_column + query_group_size * HEAD_SIZE].reshape(
            row_count * query_group_size, HEAD_SIZE
        )
        head_keys = key_block[:, kv_head * HEAD_SIZE : (kv_head + 1) * HEAD_SIZE]
        head_values = value_block[:, kv_head * HEAD_SIZE : (kv_head + 1) * HEAD_SIZE]
        scores = lax.dot_general(
            head_query, head_keys, (((1,), (1,)), ((), ())), preferred_element_type=jnp.float32
        )
        scores = (scores * score_scale).reshape(row_count, query_group_size, key_count)
        scores = jnp.where(key_mask, scores, NEGATIVE)
        row_max = jnp.max(scores, axis=2, keepdims=True)
        weights = jnp.where(key_mask, jnp.exp(scores - row_max), 0.0)
        totals = jnp.maximum(jnp.sum(weights, axis=2), 1.0)
        weighted = jnp.dot(
            weights.astype(jnp.bfloat16).reshape(row_count * query_group_size, key_count),
            head_values,
            preferred_element_type=jnp.float32,
        )
        weighted = weighted.reshape(row_count, query_group_size, HEAD_SIZE) / totals[:, :, None]
        blended_parts.append(weighted.reshape(row_count, query_group_size * HEAD_SIZE))
        lse_parts.append(row_max[:, :, 0] + jnp.log(totals))
    return (jnp.concatenate(blended_parts, axis=1), jnp.concatenate(lse_parts, axis=1))


def combine_halves(earlier, later):
    joint_max = jnp.maximum(earlier[0], later[0])
    left_factor = jnp.exp(earlier[0] - joint_max)
    right_factor = jnp.exp(later[0] - joint_max)
    totals = earlier[1] * left_factor + later[1] * right_factor
    blended = earlier[2] * left_factor[:, :, None] + later[2] * right_factor[:, :, None]
    return (joint_max, totals, blended)


def shards(
    queries,
    prompt_of,
    prompt_len,
    suffix_len,
    page_table,
    prompt_keys,
    shared_prompt_values,
    suffix_pool_keys,
    suffix_pool_values,
):
    kv_count = lax.axis_size("kv")
    sub_count = lax.axis_size("sub")
    kv_index = lax.axis_index("kv")
    sub_index = lax.axis_index("sub")
    seq_local = queries.shape[0]
    row_width = queries.shape[1]
    heads_local = row_width // HEAD_SIZE
    cache_local = prompt_keys.shape[0]
    kv_reach = sub_count * cache_local
    prompt_count = prompt_len.shape[0]
    prompt_starts = jnp.cumsum(prompt_len) - prompt_len
    prompt_ends = prompt_starts + prompt_len
    prompt_labels = jnp.arange(prompt_count, dtype=jnp.int32)
    range_low = jnp.arange(kv_count, dtype=jnp.int32) * kv_reach
    intersections = (prompt_starts[None, :] < range_low[:, None] + kv_reach) & (
        prompt_ends[None, :] > range_low[:, None]
    )
    later_slot = prompt_starts[None, :] > range_low[:, None]
    first_position = (kv_index * sub_count + sub_index) * cache_local
    most_rows = seq_local // prompt_count
    owned_prompt = lax.dynamic_slice_in_dim(prompt_of[:, 0], kv_index * seq_local, seq_local)
    prompt_hits = owned_prompt[:, None] == prompt_labels[None, :]
    hit_counts = prompt_hits.astype(jnp.int32)
    ranks = jnp.sum((jnp.cumsum(hit_counts, axis=0) - hit_counts) * hit_counts, axis=1)
    seq_intersection = jnp.any(intersections[:, None, :] & prompt_hits[None, :, :], axis=2)
    seq_later = jnp.any(later_slot[:, None, :] & prompt_hits[None, :, :], axis=2).astype(jnp.int32)
    slot_labels = jnp.arange(2, dtype=jnp.int32)
    rank_labels = jnp.arange(most_rows, dtype=jnp.int32)
    selector = seq_intersection[:, None, None, :] & (
        seq_later[:, None, None, :] == slot_labels[None, :, None, None]
    )
    selector = selector & (ranks[None, None, None, :] == rank_labels[None, None, :, None])
    selector = selector.reshape(kv_count * 2 * most_rows, seq_local)
    outgoing = jnp.dot(
        selector.astype(jnp.bfloat16), queries, preferred_element_type=jnp.float32
    ).astype(jnp.bfloat16)
    incoming = lax.all_to_all(
        outgoing.reshape(kv_count, 2 * most_rows, row_width),
        "kv",
        split_axis=0,
        concat_axis=0,
        tiled=True,
    )
    mine_intersection = lax.dynamic_index_in_dim(intersections, kv_index, 0, keepdims=False)
    mine_later = lax.dynamic_index_in_dim(later_slot, kv_index, 0, keepdims=False).astype(jnp.int32)
    chosen = mine_intersection[None, :] & (mine_later[None, :] == slot_labels[:, None])
    slot_low = jnp.sum(jnp.where(chosen, prompt_starts[None, :], 0), axis=1)
    slot_high = jnp.sum(jnp.where(chosen, prompt_ends[None, :], 0), axis=1)
    lower_bound = jnp.broadcast_to(
        jnp.repeat(slot_low, most_rows)[None, :], (kv_count, 2 * most_rows)
    ).reshape(-1)
    upper_bound = jnp.broadcast_to(
        jnp.repeat(slot_high, most_rows)[None, :], (kv_count, 2 * most_rows)
    ).reshape(-1)
    sent_rows = incoming.reshape(kv_count * 2 * most_rows, row_width)
    back_rows = 2 * most_rows
    prompt_out, prompt_lse = attend_block(
        sent_rows, prompt_keys, shared_prompt_values, lower_bound, upper_bound, first_position
    )
    returned_out, returned_lse = (
        lax.all_to_all(
            prompt_out.reshape(kv_count, back_rows, row_width),
            "kv",
            split_axis=0,
            concat_axis=0,
            tiled=True,
        ),
        lax.all_to_all(
            prompt_lse.reshape(kv_count, back_rows, heads_local),
            "kv",
            split_axis=0,
            concat_axis=0,
            tiled=True,
        ),
    )
    page_slots = page_table.shape[1]
    page_length = suffix_pool_keys.shape[1]
    suffix_span = page_slots * page_length
    gathered_keys = suffix_pool_keys[page_table].reshape(seq_local, suffix_span, -1)
    gathered_values = suffix_pool_values[page_table].reshape(seq_local, suffix_span, -1)
    suffix_first = sub_index * suffix_span

    def one_sequence(query_line, seq_keys, seq_values, seq_length):
        return attend_block(
            query_line[None, :],
            seq_keys,
            seq_values,
            jnp.zeros((1,), jnp.int32),
            seq_length[None],
            suffix_first,
        )

    suffix_out, suffix_lse = jax.vmap(one_sequence)(
        queries, gathered_keys, gathered_values, suffix_len
    )
    suffix_out = suffix_out[:, 0].reshape(seq_local, heads_local, HEAD_SIZE)
    suffix_lse = suffix_lse[:, 0]
    flat_lse = returned_lse.reshape(-1, heads_local)
    flat_out = returned_out.reshape(-1, heads_local, HEAD_SIZE)
    masked_lse = jnp.where(selector[:, :, None], flat_lse[:, None, :], NEGATIVE)
    joint_max = jnp.maximum(jnp.max(masked_lse, axis=0), suffix_lse)
    factors = jnp.where(selector[:, :, None], jnp.exp(masked_lse - joint_max[None]), 0.0)
    own_factor = jnp.exp(suffix_lse - joint_max)
    totals = jnp.sum(factors, axis=0) + own_factor
    blended = jnp.einsum("rsh,rhd->shd", factors, flat_out, precision=lax.Precision.HIGHEST)
    blended = blended + own_factor[:, :, None] * suffix_out
    joint_max, totals, blended = joined((joint_max, totals, blended), "sub", combine_halves)
    return (blended / totals[:, :, None]).reshape(seq_local, row_width).astype(jnp.float32)


SENT = jnp.int16
STEPS = 32000.0
TINY = 1e-30
LOG2E = 1.4426950408889634
FIRST_SLOT = (0, 0, 1, 1)
HOLDERS = (((0, 0), (1, 0)), ((1, 1), (2, 0), (3, 0)))
CHUNK = 4
SENDS = ((2, 0), (3, 0), (4, 0), (5, 0), (0, 0), (1, 0), (6, 0), (7, 0), (2, 1), (3, 1))


def windows(chip):
    return (0, 1) if chip == 1 else (FIRST_SLOT[chip],)


def lanes(column, width=HEAD_SIZE):
    return jnp.broadcast_to(column, (column.shape[0], width))


def attend(
    prompt_of, prompt_len, suffix_len, page_table,
    q_ref, pk_ref, pv_ref, sk_ref, sv_ref,
    out_ref,
    order, places, qf, q_send, q_all, kbuf, vbuf, pool_k, pool_v,
    o_send, l_send, o_recv, l_recv, l_cols, suf_o, suf_l, merged,
    own_sem, swap_send, swap_recv, pool_sem, qs_sem, qr_sem, os_sem, or_sem, ls_sem, lr_sem,
):
    me = lax.axis_index("kv")
    chip = me // 2
    core = me % 2
    other = 1 - core
    partner = chip * 2 + other
    devices = 8
    rows = q_ref.shape[0]
    most = rows // 2
    heads = pk_ref.shape[1] // HEAD_SIZE
    half = heads // 2
    group = q_ref.shape[1] // (heads * HEAD_SIZE)
    positions = pk_ref.shape[0]
    lines = group * most
    slots = page_table.shape[0]
    span = slots * sk_ref.shape[1]
    scale = LOG2E / math.sqrt(HEAD_SIZE)

    def columns(head):
        return pl.ds(pl.multiple_of(head * HEAD_SIZE, HEAD_SIZE), HEAD_SIZE)

    own_copies = []
    for h in range(half):
        for i, (ref, buf) in enumerate(((pk_ref, kbuf), (pv_ref, vbuf))):
            own_copies.append(pltpu.make_async_copy(
                ref.at[:, columns(core * half + h)], buf.at[core, h], own_sem.at[2 * h + i]))
    for copy in own_copies:
        copy.start()

    pool_copies = [pltpu.make_async_copy(sk_ref, pool_k, pool_sem.at[0]),
                   pltpu.make_async_copy(sv_ref, pool_v, pool_sem.at[1])]
    for copy in pool_copies:
        copy.start()

    barrier = pltpu.get_barrier_semaphore()
    for dst in range(devices):
        @pl.when(me != dst)
        def _():
            pl.semaphore_signal(barrier, inc=1, device_id={"kv": dst},
                                device_id_type=pl.DeviceIdType.MESH)

    count = [jnp.int32(0), jnp.int32(0)]
    place = []
    for s in range(rows):
        is_one = prompt_of[me * rows + s]
        place.append(jnp.where(is_one == 1, most + count[1], count[0]))
        count[0] = count[0] + (1 - is_one)
        count[1] = count[1] + is_one
        places[s] = place[s]
    row_ids = lax.broadcasted_iota(jnp.int32, (rows, rows), 0)
    col_ids = lax.broadcasted_iota(jnp.int32, (rows, rows), 1)
    chooser = jnp.zeros((rows, rows), jnp.float32)
    for s in range(rows):
        chooser = jnp.where((row_ids == place[s]) & (col_ids == s), 1.0, chooser)
    for r in range(rows):
        found = jnp.int32(0)
        for s in range(rows):
            found = jnp.where(place[s] == r, s, found)
        order[r] = found
    chooser = chooser.astype(jnp.bfloat16)
    for h in range(heads):
        width = group * HEAD_SIZE
        block = jnp.dot(chooser, q_ref[:, h * width:(h + 1) * width],
                        preferred_element_type=jnp.float32)
        for p in range(2):
            tall = jnp.concatenate(
                [block[p * most:(p + 1) * most, g * HEAD_SIZE:(g + 1) * HEAD_SIZE]
                 for g in range(group)], axis=0)
            qf[p, h] = tall
            q_send[p, h] = tall.astype(jnp.bfloat16)

    pl.semaphore_wait(barrier, devices - 1)

    def query_copy(dst, slot, src):
        c, d = dst // 2, dst % 2
        prompt = windows(c)[slot]
        return pltpu.make_async_remote_copy(
            src_ref=q_send.at[prompt, pl.ds(d * half, half)], dst_ref=q_all.at[slot, src],
            send_sem=qs_sem.at[dst, slot], recv_sem=qr_sem.at[src, slot],
            device_id={"kv": dst}, device_id_type=pl.DeviceIdType.MESH)

    for dst, slot in SENDS:
        @pl.when(me != dst)
        def _():
            query_copy(dst, slot, me).start()

        @pl.when(me == dst)
        def _():
            q_all[slot, me] = q_send[windows(dst // 2)[slot], (dst % 2) * half:(dst % 2 + 1) * half]

    def swap_copies():
        made = []
        for h in range(half):
            for i, (ref, buf) in enumerate(((pk_ref, kbuf), (pv_ref, vbuf))):
                made.append(pltpu.make_async_remote_copy(
                    src_ref=ref.at[:, columns(other * half + h)], dst_ref=buf.at[core, h],
                    send_sem=swap_send.at[2 * h + i], recv_sem=swap_recv.at[2 * h + i],
                    device_id={"kv": partner}, device_id_type=pl.DeviceIdType.MESH))
        return made

    swaps = swap_copies()
    for copy in swaps:
        copy.start()

    for copy in own_copies:
        copy.wait()
    for copy in swaps:
        copy.wait_recv()

    first_end = prompt_len[0]
    second_end = first_end + prompt_len[1]

    def wait_query(src, slot):
        pltpu.make_async_remote_copy(
            src_ref=q_send.at[0, pl.ds(0, half)], dst_ref=q_all.at[slot, src],
            send_sem=qs_sem.at[src, slot], recv_sem=qr_sem.at[src, slot],
            device_id={"kv": src}, device_id_type=pl.DeviceIdType.MESH).wait_recv()

    side = me // CHUNK

    def back_copies(dst, slot, sender):
        return (
            pltpu.make_async_remote_copy(
                src_ref=o_send.at[slot, dst], dst_ref=o_recv.at[slot, sender],
                send_sem=os_sem.at[dst, slot], recv_sem=or_sem.at[sender, slot],
                device_id={"kv": dst}, device_id_type=pl.DeviceIdType.MESH),
            pltpu.make_async_remote_copy(
                src_ref=l_send.at[slot, dst], dst_ref=l_recv.at[slot, sender],
                send_sem=ls_sem.at[dst, slot], recv_sem=lr_sem.at[sender, slot],
                device_id={"kv": dst}, device_id_type=pl.DeviceIdType.MESH))

    def prompt_slot(slot, low, high, first_block):
        blocks = 2 - first_block
        spot = (chip * 2 + first_block) * positions + lax.broadcasted_iota(
            jnp.int32, (1, blocks * positions), 1)
        bias = jnp.where((spot >= low) & (spot < high), 0.0, NEGATIVE)
        is_level = lax.broadcasted_iota(jnp.int32, (CHUNK * lines, HEAD_SIZE), 1) % 8 < 4

        @pl.loop(0, devices // CHUNK)
        def _(turn):
            near = (turn == 0) if slot == 0 else (turn == 1)
            begin = jnp.where(near, side, 1 - side) * CHUNK

            @pl.loop(0, CHUNK)
            def _(offset):
                src = begin + offset

                @pl.when(me != src)
                def _():
                    wait_query(src, slot)

            @pl.loop(0, half, unroll=2)
            def _(h):
                query = q_all[slot, pl.ds(begin, CHUNK), h].reshape(CHUNK * lines, HEAD_SIZE)
                keys = kbuf[first_block:2, h].reshape(blocks * positions, HEAD_SIZE)
                values = vbuf[first_block:2, h].reshape(blocks * positions, HEAD_SIZE)
                scores = lax.dot_general(query, keys, (((1,), (1,)), ((), ())),
                                         preferred_element_type=jnp.float32)
                scores = scores * scale + bias
                top = jnp.max(scores, axis=1, keepdims=True)
                weights = jnp.exp2(scores - top)
                total = jnp.sum(weights, axis=1, keepdims=True)
                mixed = jnp.dot(weights.astype(jnp.bfloat16), values,
                                preferred_element_type=jnp.float32)
                peak = jnp.maximum(jnp.max(jnp.abs(mixed), axis=1, keepdims=True), TINY)
                steps = jnp.round(mixed * (STEPS / peak)).astype(jnp.int32)
                o_send[slot, pl.ds(begin, CHUNK), h] = steps.astype(SENT).reshape(
                    CHUNK, lines, HEAD_SIZE)
                peak = peak * (1.0 / (STEPS * total))
                facts = jnp.where(is_level, lanes(top + jnp.log2(total)), lanes(peak))
                l_cols[pl.ds(begin, CHUNK), h] = facts.reshape(CHUNK, lines, HEAD_SIZE)

            @pl.loop(0, CHUNK)
            def _(offset):
                dst = begin + offset
                turned = l_cols[dst].reshape(half * lines, HEAD_SIZE).T
                l_send[slot, dst] = turned[0:8]

                @pl.when(me != dst)
                def _():
                    for copy in back_copies(dst, slot, me):
                        copy.start()

                @pl.when(me == dst)
                def _():
                    o_recv[slot, me] = o_send[slot, dst]
                    l_recv[slot, me] = l_send[slot, dst]

    prompt_slot(0, jnp.where(chip < 2, 0, first_end), jnp.where(chip < 2, first_end, second_end), 0)

    @pl.when(chip == 1)
    def _():
        prompt_slot(1, first_end, second_end, 1)

    for copy in pool_copies:
        copy.wait()
    suffix_spot = lax.broadcasted_iota(jnp.int32, (1, span), 1)
    zero = jnp.zeros((group, HEAD_SIZE), jnp.float32)

    @pl.loop(0, rows, unroll=4)
    def _(r):
        s = order[r]
        p, rank = r // most, r % most
        every = pl.ds(rank, group, stride=most)
        wide = []
        for h in range(heads):
            piece = qf[p, h, every, :]
            wide.append(jnp.concatenate([zero] * h + [piece] + [zero] * (heads - 1 - h), axis=1))
        query = jnp.concatenate(wide, axis=0).astype(jnp.bfloat16)
        keys = jnp.concatenate([pool_k[page_table[j, s]] for j in range(slots)], axis=0)
        values = jnp.concatenate([pool_v[page_table[j, s]] for j in range(slots)], axis=0)
        scores = lax.dot_general(query, keys, (((1,), (1,)), ((), ())),
                                 preferred_element_type=jnp.float32)
        scores = scores * scale + jnp.where(suffix_spot < suffix_len[s], 0.0, NEGATIVE)
        top = jnp.max(scores, axis=1, keepdims=True)
        weights = jnp.exp2(scores - top)
        total = jnp.sum(weights, axis=1, keepdims=True)
        mixed = jnp.dot(weights.astype(jnp.bfloat16), values, preferred_element_type=jnp.float32)
        inverse = 1.0 / total
        lse = top + jnp.log2(total)
        for h in range(heads):
            low = h * group
            suf_o[p, h, every, :] = (
                mixed[low:low + group, h * HEAD_SIZE:(h + 1) * HEAD_SIZE] * inverse[low:low + group])
            suf_l[p, h, every, :] = lanes(lse[low:low + group])

    for p in range(2):
        for d in range(2):
            arrived, levels = [], []
            for c, slot in HOLDERS[p]:
                sender = 2 * c + d

                @pl.when(me != sender)
                def _():
                    for copy in back_copies(sender, slot, sender):
                        copy.wait_recv()

                facts = l_recv[slot, sender]
                facts = jnp.concatenate([facts] * (HEAD_SIZE // 8), axis=0).T
                levels.append((lanes(facts[:, 0:1]), lanes(facts[:, 4:5])))
                arrived.append((slot, sender))
            for hh in range(half):
                h = d * half + hh
                mine = slice(hh * lines, (hh + 1) * lines)
                parts = [(level[mine], o_recv[slot, sender, hh].astype(jnp.int32).astype(jnp.float32)
                          * step[mine])
                         for (level, step), (slot, sender) in zip(levels, arrived)]
                parts.append((suf_l[p, h], suf_o[p, h]))
                joint = functools.reduce(jnp.maximum, [level for level, _ in parts])
                factors = [jnp.exp2(level - joint) for level, _ in parts]
                total = functools.reduce(jnp.add, factors)
                blend = functools.reduce(jnp.add, [f * o for f, (_, o) in zip(factors, parts)])
                blend = blend / total
                for g in range(group):
                    first = (h * group + g) * HEAD_SIZE
                    merged[p * most:(p + 1) * most, first:first + HEAD_SIZE] = (
                        blend[g * most:(g + 1) * most])

    for s in range(rows):
        out_ref[s:s + 1, :] = merged[pl.ds(places[s], 1), :]

    for copy in swaps:
        copy.wait_send()


    for dst in range(devices):
        @pl.when(me != dst)
        def _():
            for slot in range(len(windows(dst // 2))):
                query_copy(dst, slot, me).wait_send()

        @pl.when(me != dst)
        def _():
            for copy in back_copies(dst, 0, me):
                copy.wait_send()

        @pl.when((me != dst) & (chip == 1))
        def _():
            for copy in back_copies(dst, 1, me):
                copy.wait_send()


def fused(
    queries,
    prompt_of,
    prompt_len,
    suffix_len,
    page_table,
    prompt_keys,
    shared_prompt_values,
    suffix_pool_keys,
    suffix_pool_values,
):
    rows, width = queries.shape
    most = rows // 2
    positions, depth = prompt_keys.shape
    heads = depth // HEAD_SIZE
    half = heads // 2
    group = width // depth
    lines = group * most
    devices = lax.axis_size("kv")
    f32, bf16 = jnp.float32, jnp.bfloat16
    vmem, dma = pltpu.VMEM, pltpu.SemaphoreType.DMA
    return pl.pallas_call(
        attend,
        out_shape=pltpu.VMEM((rows, width), f32),
        in_specs=[pl.BlockSpec(memory_space=pltpu.SMEM)] * 4
        + [pl.BlockSpec(memory_space=pltpu.VMEM)]
        + [pl.BlockSpec(memory_space=pl.ANY)] * 4,
        out_specs=pl.BlockSpec(memory_space=pltpu.VMEM),
        scratch_shapes=[
            pltpu.SMEM((rows,), jnp.int32),
            pltpu.SMEM((rows,), jnp.int32),
            vmem((2, heads, lines, HEAD_SIZE), f32),
            vmem((2, heads, lines, HEAD_SIZE), bf16),
            vmem((2, devices, half, lines, HEAD_SIZE), bf16),
            vmem((2, half, positions, HEAD_SIZE), bf16),
            vmem((2, half, positions, HEAD_SIZE), bf16),
            vmem(suffix_pool_keys.shape, bf16),
            vmem(suffix_pool_values.shape, bf16),
            vmem((2, devices, half, lines, HEAD_SIZE), SENT),
            vmem((2, devices, 8, HEAD_SIZE), f32),
            vmem((2, devices, half, lines, HEAD_SIZE), SENT),
            vmem((2, devices, 8, HEAD_SIZE), f32),
            vmem((devices, half, lines, HEAD_SIZE), f32),
            vmem((2, heads, lines, HEAD_SIZE), f32),
            vmem((2, heads, lines, HEAD_SIZE), f32),
            vmem((rows, width), f32),
            dma((2 * half,)),
            dma((2 * half,)),
            dma((2 * half,)),
            dma((2,)),
            dma((devices, 2)),
            dma((devices, 2)),
            dma((devices, 2)),
            dma((devices, 2)),
            dma((devices, 2)),
            dma((devices, 2)),
        ],
        compiler_params=pltpu.CompilerParams(
            collective_id=0, has_side_effects=True, vmem_limit_bytes=48 * 1024 * 1024
        ),
    )(
        *(pltpu.with_memory_space_constraint(array, pltpu.HBM) for array in (
            prompt_of.reshape(-1), prompt_len, suffix_len, page_table.T,
            queries, prompt_keys, shared_prompt_values, suffix_pool_keys, suffix_pool_values))
    )


def fits(mesh):
    return mesh.shape["kv"] == 8 and mesh.shape["sub"] == 1


def solution(mesh):
    body = fused if fits(mesh) else shards
    placed = (
        P(("grp", "kv"), "hd"),
        P("grp", None),
        P("grp"),
        P(("grp", "kv")),
        P(("grp", "kv"), "sub"),
        P(("grp", "kv", "sub"), "hd"),
        P(("grp", "kv", "sub"), "hd"),
        P(("grp", "kv", "sub"), None, "hd"),
        P(("grp", "kv", "sub"), None, "hd"),
    )
    return jax.shard_map(
        body, mesh=mesh, in_specs=placed, out_specs=P(("grp", "kv"), "hd"), check_vma=False
    )
```

```python
import functools
import math

import jax
import jax.numpy as jnp
from jax import lax
from jax.experimental import pallas as pl
from jax.experimental.pallas import tpu as pltpu
from jax.sharding import PartitionSpec as P

HEAD_SIZE = 128


NEGATIVE = -1e30


def joined(value, axis, combine):
    everything = jax.tree.map(lambda part: lax.all_gather(part, axis), value)
    leading = jax.tree.map(lambda part: part[0], everything)

    def hop(k, so_far):
        return combine(so_far, jax.tree.map(lambda part: part[k], everything))

    return lax.fori_loop(1, lax.axis_size(axis), hop, leading)


def attend_block(sent_rows, key_block, value_block, lower_bound, upper_bound, first_position):
    row_count = sent_rows.shape[0]
    key_count = key_block.shape[0]
    kv_local = key_block.shape[1] // HEAD_SIZE
    query_group_size = sent_rows.shape[1] // (HEAD_SIZE * kv_local)
    position = first_position + jnp.arange(key_count, dtype=jnp.int32)
    key_mask = (position[None, :] >= lower_bound[:, None]) & (
        position[None, :] < upper_bound[:, None]
    )
    key_mask = key_mask[:, None, :]
    score_scale = 1.0 / math.sqrt(HEAD_SIZE)
    blended_parts = []
    lse_parts = []
    for kv_head in range(kv_local):
        low_column = kv_head * query_group_size * HEAD_SIZE
        head_query = sent_rows[:, low_column : low_column + query_group_size * HEAD_SIZE].reshape(
            row_count * query_group_size, HEAD_SIZE
        )
        head_keys = key_block[:, kv_head * HEAD_SIZE : (kv_head + 1) * HEAD_SIZE]
        head_values = value_block[:, kv_head * HEAD_SIZE : (kv_head + 1) * HEAD_SIZE]
        scores = lax.dot_general(
            head_query, head_keys, (((1,), (1,)), ((), ())), preferred_element_type=jnp.float32
        )
        scores = (scores * score_scale).reshape(row_count, query_group_size, key_count)
        scores = jnp.where(key_mask, scores, NEGATIVE)
        row_max = jnp.max(scores, axis=2, keepdims=True)
        weights = jnp.where(key_mask, jnp.exp(scores - row_max), 0.0)
        totals = jnp.maximum(jnp.sum(weights, axis=2), 1.0)
        weighted = jnp.dot(
            weights.astype(jnp.bfloat16).reshape(row_count * query_group_size, key_count),
            head_values,
            preferred_element_type=jnp.float32,
        )
        weighted = weighted.reshape(row_count, query_group_size, HEAD_SIZE) / totals[:, :, None]
        blended_parts.append(weighted.reshape(row_count, query_group_size * HEAD_SIZE))
        lse_parts.append(row_max[:, :, 0] + jnp.log(totals))
    return (jnp.concatenate(blended_parts, axis=1), jnp.concatenate(lse_parts, axis=1))


def combine_halves(earlier, later):
    joint_max = jnp.maximum(earlier[0], later[0])
    left_factor = jnp.exp(earlier[0] - joint_max)
    right_factor = jnp.exp(later[0] - joint_max)
    totals = earlier[1] * left_factor + later[1] * right_factor
    blended = earlier[2] * left_factor[:, :, None] + later[2] * right_factor[:, :, None]
    return (joint_max, totals, blended)


def shards(
    queries,
    prompt_of,
    prompt_len,
    suffix_len,
    page_table,
    prompt_keys,
    shared_prompt_values,
    suffix_pool_keys,
    suffix_pool_values,
):
    kv_count = lax.axis_size("kv")
    sub_count = lax.axis_size("sub")
    kv_index = lax.axis_index("kv")
    sub_index = lax.axis_index("sub")
    seq_local = queries.shape[0]
    row_width = queries.shape[1]
    heads_local = row_width // HEAD_SIZE
    cache_local = prompt_keys.shape[0]
    kv_reach = sub_count * cache_local
    prompt_count = prompt_len.shape[0]
    prompt_starts = jnp.cumsum(prompt_len) - prompt_len
    prompt_ends = prompt_starts + prompt_len
    prompt_labels = jnp.arange(prompt_count, dtype=jnp.int32)
    range_low = jnp.arange(kv_count, dtype=jnp.int32) * kv_reach
    intersections = (prompt_starts[None, :] < range_low[:, None] + kv_reach) & (
        prompt_ends[None, :] > range_low[:, None]
    )
    later_slot = prompt_starts[None, :] > range_low[:, None]
    first_position = (kv_index * sub_count + sub_index) * cache_local
    most_rows = seq_local // prompt_count
    owned_prompt = lax.dynamic_slice_in_dim(prompt_of[:, 0], kv_index * seq_local, seq_local)
    prompt_hits = owned_prompt[:, None] == prompt_labels[None, :]
    hit_counts = prompt_hits.astype(jnp.int32)
    ranks = jnp.sum((jnp.cumsum(hit_counts, axis=0) - hit_counts) * hit_counts, axis=1)
    seq_intersection = jnp.any(intersections[:, None, :] & prompt_hits[None, :, :], axis=2)
    seq_later = jnp.any(later_slot[:, None, :] & prompt_hits[None, :, :], axis=2).astype(jnp.int32)
    slot_labels = jnp.arange(2, dtype=jnp.int32)
    rank_labels = jnp.arange(most_rows, dtype=jnp.int32)
    selector = seq_intersection[:, None, None, :] & (
        seq_later[:, None, None, :] == slot_labels[None, :, None, None]
    )
    selector = selector & (ranks[None, None, None, :] == rank_labels[None, None, :, None])
    selector = selector.reshape(kv_count * 2 * most_rows, seq_local)
    outgoing = jnp.dot(
        selector.astype(jnp.bfloat16), queries, preferred_element_type=jnp.float32
    ).astype(jnp.bfloat16)
    incoming = lax.all_to_all(
        outgoing.reshape(kv_count, 2 * most_rows, row_width),
        "kv",
        split_axis=0,
        concat_axis=0,
        tiled=True,
    )
    mine_intersection = lax.dynamic_index_in_dim(intersections, kv_index, 0, keepdims=False)
    mine_later = lax.dynamic_index_in_dim(later_slot, kv_index, 0, keepdims=False).astype(jnp.int32)
    chosen = mine_intersection[None, :] & (mine_later[None, :] == slot_labels[:, None])
    slot_low = jnp.sum(jnp.where(chosen, prompt_starts[None, :], 0), axis=1)
    slot_high = jnp.sum(jnp.where(chosen, prompt_ends[None, :], 0), axis=1)
    lower_bound = jnp.broadcast_to(
        jnp.repeat(slot_low, most_rows)[None, :], (kv_count, 2 * most_rows)
    ).reshape(-1)
    upper_bound = jnp.broadcast_to(
        jnp.repeat(slot_high, most_rows)[None, :], (kv_count, 2 * most_rows)
    ).reshape(-1)
    sent_rows = incoming.reshape(kv_count * 2 * most_rows, row_width)
    back_rows = 2 * most_rows
    prompt_out, prompt_lse = attend_block(
        sent_rows, prompt_keys, shared_prompt_values, lower_bound, upper_bound, first_position
    )
    returned_out, returned_lse = (
        lax.all_to_all(
            prompt_out.reshape(kv_count, back_rows, row_width),
            "kv",
            split_axis=0,
            concat_axis=0,
            tiled=True,
        ),
        lax.all_to_all(
            prompt_lse.reshape(kv_count, back_rows, heads_local),
            "kv",
            split_axis=0,
            concat_axis=0,
            tiled=True,
        ),
    )
    page_slots = page_table.shape[1]
    page_length = suffix_pool_keys.shape[1]
    suffix_span = page_slots * page_length
    gathered_keys = suffix_pool_keys[page_table].reshape(seq_local, suffix_span, -1)
    gathered_values = suffix_pool_values[page_table].reshape(seq_local, suffix_span, -1)
    suffix_first = sub_index * suffix_span

    def one_sequence(query_line, seq_keys, seq_values, seq_length):
        return attend_block(
            query_line[None, :],
            seq_keys,
            seq_values,
            jnp.zeros((1,), jnp.int32),
            seq_length[None],
            suffix_first,
        )

    suffix_out, suffix_lse = jax.vmap(one_sequence)(
        queries, gathered_keys, gathered_values, suffix_len
    )
    suffix_out = suffix_out[:, 0].reshape(seq_local, heads_local, HEAD_SIZE)
    suffix_lse = suffix_lse[:, 0]
    flat_lse = returned_lse.reshape(-1, heads_local)
    flat_out = returned_out.reshape(-1, heads_local, HEAD_SIZE)
    masked_lse = jnp.where(selector[:, :, None], flat_lse[:, None, :], NEGATIVE)
    joint_max = jnp.maximum(jnp.max(masked_lse, axis=0), suffix_lse)
    factors = jnp.where(selector[:, :, None], jnp.exp(masked_lse - joint_max[None]), 0.0)
    own_factor = jnp.exp(suffix_lse - joint_max)
    totals = jnp.sum(factors, axis=0) + own_factor
    blended = jnp.einsum("rsh,rhd->shd", factors, flat_out, precision=lax.Precision.HIGHEST)
    blended = blended + own_factor[:, :, None] * suffix_out
    joint_max, totals, blended = joined((joint_max, totals, blended), "sub", combine_halves)
    return (blended / totals[:, :, None]).reshape(seq_local, row_width).astype(jnp.float32)


SENT = jnp.int16
STEPS = 32000.0
TINY = 1e-30
LOG2E = 1.4426950408889634
FIRST_SLOT = (0, 0, 1, 1)
HOLDERS = (((0, 0), (1, 0)), ((1, 1), (2, 0), (3, 0)))
CHUNK = 4
SENDS = ((2, 0), (3, 0), (2, 1), (3, 1), (0, 0), (1, 0), (4, 0), (5, 0), (6, 0), (7, 0))


def windows(chip):
    return (0, 1) if chip == 1 else (FIRST_SLOT[chip],)


def lanes(column, width=HEAD_SIZE):
    return jnp.broadcast_to(column, (column.shape[0], width))


def standing(row):
    return jnp.broadcast_to(row, (HEAD_SIZE, HEAD_SIZE)).T


def attend(
    of_ref, len_ref, suf_ref, table_ref, q_in, pk_ref, pv_ref, sk_ref, sv_ref,
    out_ref,
    prompt_of, prompt_len, suffix_len, page_table, q_ref, order, places, qf, q_send, q_all, kbuf, vbuf, pool_k, pool_v,
    o_send, l_send, o_recv, l_recv, l_cols, suf_w, suf_s, suf_o, suf_l, merged,
    in_sem, own_sem, swap_send, swap_recv, pool_sem, qs_sem, qr_sem, os_sem, or_sem, ls_sem, lr_sem,
    ready_sem,
):
    me = lax.axis_index("kv")
    chip = me // 2
    core = me % 2
    other = 1 - core
    partner = chip * 2 + other
    devices = 8
    rows = q_ref.shape[0]
    most = rows // 2
    heads = pk_ref.shape[1] // HEAD_SIZE
    half = heads // 2
    group = q_ref.shape[1] // (heads * HEAD_SIZE)
    positions = pk_ref.shape[0]
    lines = group * most
    slots = page_table.shape[0]
    span = slots * sk_ref.shape[1]
    scale = LOG2E / math.sqrt(HEAD_SIZE)

    def columns(head):
        return pl.ds(pl.multiple_of(head * HEAD_SIZE, HEAD_SIZE), HEAD_SIZE)

    def signal(semaphore, dst):
        pl.semaphore_signal(semaphore, inc=1, device_id={"kv": dst},
                            device_id_type=pl.DeviceIdType.MESH)

    barrier = pltpu.get_barrier_semaphore()
    for dst in range(devices):
        @pl.when((dst == partner) | (dst // 2 > chip))
        def _():
            signal(barrier, dst)

    pool_copies = [pltpu.make_async_copy(sk_ref, pool_k, pool_sem.at[0]),
                   pltpu.make_async_copy(sv_ref, pool_v, pool_sem.at[1])]
    own_copies = []
    for h in range(half):
        for i, (ref, buf) in enumerate(((pk_ref, kbuf), (pv_ref, vbuf))):
            own_copies.append(pltpu.make_async_copy(
                ref.at[:, columns(core * half + h)], buf.at[core, h], own_sem.at[2 * h + i]))
    inputs = [pltpu.make_async_copy(src, dst, in_sem.at[i]) for i, (src, dst) in enumerate((
        (of_ref, prompt_of), (len_ref, prompt_len), (suf_ref, suffix_len),
        (table_ref, page_table), (q_in, q_ref)))]
    for copy in inputs:
        copy.start()
    pool_copies[0].start()
    for copy in own_copies:
        copy.start()
    pl.semaphore_wait(barrier, 2 * chip + 1)
    for dst in range(devices):
        @pl.when(dst // 2 < chip)
        def _():
            signal(ready_sem.at[chip], dst)

    def swap_copies():
        made = []
        for h in range(half):
            for i, (ref, buf) in enumerate(((pk_ref, kbuf), (pv_ref, vbuf))):
                made.append(pltpu.make_async_remote_copy(
                    src_ref=ref.at[:, columns(other * half + h)], dst_ref=buf.at[core, h],
                    send_sem=swap_send.at[2 * h + i], recv_sem=swap_recv.at[2 * h + i],
                    device_id={"kv": partner}, device_id_type=pl.DeviceIdType.MESH))
        return made

    swaps = swap_copies()
    for copy in swaps:
        copy.start()

    for copy in inputs:
        copy.wait()

    count = [jnp.int32(0), jnp.int32(0)]
    place = []
    for s in range(rows):
        is_one = prompt_of[me * rows + s]
        place.append(jnp.where(is_one == 1, most + count[1], count[0]))
        count[0] = count[0] + (1 - is_one)
        count[1] = count[1] + is_one
        places[s] = place[s]
    row_ids = lax.broadcasted_iota(jnp.int32, (rows, rows), 0)
    col_ids = lax.broadcasted_iota(jnp.int32, (rows, rows), 1)
    chooser = jnp.zeros((rows, rows), jnp.float32)
    for s in range(rows):
        chooser = jnp.where((row_ids == place[s]) & (col_ids == s), 1.0, chooser)
    for r in range(rows):
        found = jnp.int32(0)
        for s in range(rows):
            found = jnp.where(place[s] == r, s, found)
        order[r] = found
    chooser = chooser.astype(jnp.bfloat16)

    for h in range(heads):
        width = group * HEAD_SIZE
        block = jnp.dot(chooser, q_ref[:, h * width:(h + 1) * width],
                        preferred_element_type=jnp.float32)
        for p in range(2):
            tall = jnp.concatenate(
                [block[p * most:(p + 1) * most, g * HEAD_SIZE:(g + 1) * HEAD_SIZE]
                 for g in range(group)], axis=0)
            qf[p, h] = tall
            q_send[p, h] = tall.astype(jnp.bfloat16)

    def query_copy(dst, slot, src):
        prompt = windows(dst // 2)[slot]
        return pltpu.make_async_remote_copy(
            src_ref=q_send.at[prompt, pl.ds(dst % 2 * half, half)], dst_ref=q_all.at[slot, src],
            send_sem=qs_sem.at[dst, slot], recv_sem=qr_sem.at[src, slot],
            device_id={"kv": dst}, device_id_type=pl.DeviceIdType.MESH)

    def send_up(to):
        pl.semaphore_wait(ready_sem.at[to], 2)
        for dst, slot in SENDS:
            if dst // 2 == to:
                query_copy(dst, slot, me).start()

    for dst, slot in SENDS:
        @pl.when((me != dst) & (dst // 2 <= chip))
        def _():
            query_copy(dst, slot, me).start()

        @pl.when(me == dst)
        def _():
            q_all[slot, me] = q_send[windows(dst // 2)[slot], (dst % 2) * half:(dst % 2 + 1) * half]

    @pl.when(chip == 0)
    def _():
        send_up(1)

    @pl.when(chip == 1)
    def _():
        send_up(2)

    @pl.when((chip == 1) | (chip == 2))
    def _():
        send_up(3)

    spots = lax.broadcasted_iota(jnp.int32, (span, HEAD_SIZE), 0)
    lane = lax.broadcasted_iota(jnp.int32, (1, HEAD_SIZE), 1)
    pairs = heads // 2

    def gathered(pool, s, columns_of):
        return jnp.concatenate(
            [pool[page_table[j, s], :, columns_of] for j in range(slots)], axis=0)

    pool_copies[0].wait()
    pool_copies[1].start()

    def suffix_scores(batch):
        p, pair = batch // pairs, batch % pairs
        wanted = pl.ds(pl.multiple_of(pair * 2 * HEAD_SIZE, 2 * HEAD_SIZE), 2 * HEAD_SIZE)
        tall = qf[p, pl.ds(pair * 2, 2)].reshape(2 * lines, HEAD_SIZE).T.astype(jnp.bfloat16)
        scores = None
        length = jnp.zeros((1, HEAD_SIZE), jnp.int32)
        for rank in range(most):
            s = order[p * most + rank]
            mine = lane % most == rank
            length = jnp.where(mine, suffix_len[s], length)
            both = [jnp.where(mine & (lane // lines == i), 1.0, 0.0).astype(jnp.bfloat16)
                    for i in range(2)]
            query = jnp.concatenate([tall * both[0], tall * both[1]], axis=0)
            part = jnp.dot(gathered(pool_k, s, wanted), query, preferred_element_type=jnp.float32)
            scores = part if scores is None else scores + part
        scores = jnp.where(spots < length, scores * scale, NEGATIVE)
        top = jnp.max(scores, axis=0, keepdims=True)
        weights = jnp.exp2(scores - top)
        total = jnp.sum(weights, axis=0, keepdims=True)
        suf_w[batch] = weights.T.astype(jnp.bfloat16)
        suf_s[batch, 0:1] = top + jnp.log2(total)
        suf_s[batch, 1:2] = 1.0 / total

    @pl.loop(0, 2)
    def _(p):
        for pair in range(pairs):
            suffix_scores(p * pairs + pair)

        @pl.when((chip == 0) & (p == 0))
        def _():
            for to in (2, 3):
                send_up(to)


    for copy in own_copies:
        copy.wait()
    for copy in swaps:
        copy.wait_recv()

    first_end = prompt_len[0]
    second_end = first_end + prompt_len[1]

    def wait_query(src, slot):
        pltpu.make_async_remote_copy(
            src_ref=q_send.at[0, pl.ds(0, half)], dst_ref=q_all.at[slot, src],
            send_sem=qs_sem.at[src, slot], recv_sem=qr_sem.at[src, slot],
            device_id={"kv": src}, device_id_type=pl.DeviceIdType.MESH).wait_recv()

    def back_copies(dst, slot, sender):
        return (
            pltpu.make_async_remote_copy(
                src_ref=o_send.at[slot, dst], dst_ref=o_recv.at[slot, sender],
                send_sem=os_sem.at[dst, slot], recv_sem=or_sem.at[sender, slot],
                device_id={"kv": dst}, device_id_type=pl.DeviceIdType.MESH),
            pltpu.make_async_remote_copy(
                src_ref=l_send.at[slot, dst], dst_ref=l_recv.at[slot, sender],
                send_sem=ls_sem.at[dst, slot], recv_sem=lr_sem.at[sender, slot],
                device_id={"kv": dst}, device_id_type=pl.DeviceIdType.MESH))

    is_level = lax.broadcasted_iota(jnp.int32, (CHUNK * lines, HEAD_SIZE), 1) % 2 == 0

    def prompt_turn(slot, turn, low, high, first_block):
        blocks = 2 - first_block
        spot = (chip * 2 + first_block) * positions + lax.broadcasted_iota(
            jnp.int32, (1, blocks * positions), 1)
        bias = jnp.where((spot >= low) & (spot < high), 0.0, NEGATIVE)
        begin = turn * CHUNK

        @pl.loop(0, CHUNK)
        def _(offset):
            src = begin + offset

            @pl.when(me != src)
            def _():
                wait_query(src, slot)

        @pl.loop(0, half, unroll=2)
        def _(h):
            query = q_all[slot, pl.ds(begin, CHUNK), h].reshape(CHUNK * lines, HEAD_SIZE)
            keys = kbuf[first_block:2, h].reshape(blocks * positions, HEAD_SIZE)
            values = vbuf[first_block:2, h].reshape(blocks * positions, HEAD_SIZE)
            scores = lax.dot_general(query, keys, (((1,), (1,)), ((), ())),
                                     preferred_element_type=jnp.float32)
            scores = scores * scale + bias
            top = jnp.max(scores, axis=1, keepdims=True)
            weights = jnp.exp2(scores - top)
            total = jnp.sum(weights, axis=1, keepdims=True)
            mixed = jnp.dot(weights.astype(jnp.bfloat16), values,
                            preferred_element_type=jnp.float32)
            peak = jnp.maximum(jnp.max(jnp.abs(mixed), axis=1, keepdims=True), TINY)
            steps = jnp.round(mixed * (STEPS / peak)).astype(jnp.int32)
            o_send[slot, pl.ds(begin, CHUNK), h] = steps.astype(SENT).reshape(
                CHUNK, lines, HEAD_SIZE)
            peak = peak * (1.0 / (STEPS * total))
            facts = jnp.where(is_level, lanes(top + jnp.log2(total)), lanes(peak))
            l_cols[pl.ds(begin, CHUNK), h] = facts.reshape(CHUNK, lines, HEAD_SIZE)

        @pl.loop(0, CHUNK)
        def _(offset):
            dst = begin + offset
            turned = l_cols[dst].reshape(half * lines, HEAD_SIZE).T
            l_send[slot, dst] = turned[0:2]

            @pl.when(me != dst)
            def _():
                for copy in back_copies(dst, slot, me):
                    copy.start()

            @pl.when(me == dst)
            def _():
                o_recv[slot, me] = o_send[slot, dst]
                l_recv[slot, me] = l_send[slot, dst]

    low, high = jnp.where(chip < 2, 0, first_end), jnp.where(chip < 2, first_end, second_end)
    row = lax.broadcasted_iota(jnp.int32, (2 * lines, HEAD_SIZE), 0)
    late = jnp.where(chip == 1, 1, 0)

    @pl.loop(0, devices // CHUNK)
    def _(step):
        turn = jnp.where(chip == 1, 1 - step, step)
        prompt_turn(0, turn, low, high, 0)

        @pl.when(chip == 1)
        def _():
            prompt_turn(1, turn, first_end, second_end, 1)

        @pl.when(step == late)
        def _():
            pool_copies[1].wait()

            @pl.loop(0, 2 * pairs)
            def _(batch):
                p, pair = batch // pairs, batch % pairs
                wanted = pl.ds(pl.multiple_of(pair * 2 * HEAD_SIZE, 2 * HEAD_SIZE), 2 * HEAD_SIZE)
                weights = suf_w[batch]
                mixed = None
                for rank in range(most):
                    s = order[p * most + rank]
                    mine = jnp.where(row % most == rank, 1.0, 0.0).astype(jnp.bfloat16)
                    mine = jnp.concatenate([mine] * (span // HEAD_SIZE), axis=1)
                    part = jnp.dot(weights * mine, gathered(pool_v, s, wanted),
                                   preferred_element_type=jnp.float32)
                    mixed = part if mixed is None else mixed + part
                level, inverse = standing(suf_s[batch, 0:1]), standing(suf_s[batch, 1:2])
                for i in range(2):
                    mine = slice(i * lines, (i + 1) * lines)
                    suf_o[p, pair * 2 + i] = (
                        mixed[mine, i * HEAD_SIZE:(i + 1) * HEAD_SIZE] * inverse[mine])
                    suf_l[p, pair * 2 + i] = level[mine]

    for p in range(2):
        for d in range(2):
            arrived, levels = [], []
            for c, slot in HOLDERS[p]:
                sender = 2 * c + d

                @pl.when(me != sender)
                def _():
                    for copy in back_copies(sender, slot, sender):
                        copy.wait_recv()

                levels.append((standing(l_recv[slot, sender, 0:1]), standing(l_recv[slot, sender, 1:2])))
                arrived.append((slot, sender))
            for hh in range(half):
                h = d * half + hh
                mine = slice(hh * lines, (hh + 1) * lines)
                parts = [(level[mine], o_recv[slot, sender, hh].astype(jnp.int32).astype(jnp.float32)
                          * step[mine])
                         for (level, step), (slot, sender) in zip(levels, arrived)]
                parts.append((suf_l[p, h], suf_o[p, h]))
                joint = functools.reduce(jnp.maximum, [level for level, _ in parts])
                factors = [jnp.exp2(level - joint) for level, _ in parts]
                total = functools.reduce(jnp.add, factors)
                blend = functools.reduce(jnp.add, [f * o for f, (_, o) in zip(factors, parts)])
                blend = blend / total
                for g in range(group):
                    first = (h * group + g) * HEAD_SIZE
                    merged[p * most:(p + 1) * most, first:first + HEAD_SIZE] = (
                        blend[g * most:(g + 1) * most])

    for s in range(rows):
        out_ref[s:s + 1, :] = merged[pl.ds(places[s], 1), :]

    for copy in swaps:
        copy.wait_send()

    for dst, slot in SENDS:
        @pl.when((me != dst))
        def _():
            query_copy(dst, slot, me).wait_send()

    for dst in range(devices):
        @pl.when(me != dst)
        def _():
            for copy in back_copies(dst, 0, me):
                copy.wait_send()

        @pl.when((me != dst) & (chip == 1))
        def _():
            for copy in back_copies(dst, 1, me):
                copy.wait_send()


def fused(
    queries,
    prompt_of,
    prompt_len,
    suffix_len,
    page_table,
    prompt_keys,
    shared_prompt_values,
    suffix_pool_keys,
    suffix_pool_values,
):
    rows, width = queries.shape
    most = rows // 2
    positions, depth = prompt_keys.shape
    heads = depth // HEAD_SIZE
    half = heads // 2
    group = width // depth
    lines = group * most
    span = page_table.shape[1] * suffix_pool_keys.shape[1]
    devices = lax.axis_size("kv")
    f32, bf16 = jnp.float32, jnp.bfloat16
    vmem, dma = pltpu.VMEM, pltpu.SemaphoreType.DMA
    return pl.pallas_call(
        attend,
        out_shape=pltpu.VMEM((rows, width), f32),
        in_specs=[pl.BlockSpec(memory_space=pl.ANY)] * 9,
        out_specs=pl.BlockSpec(memory_space=pltpu.VMEM),
        scratch_shapes=[
            pltpu.SMEM(prompt_of.shape[:1], jnp.int32),
            pltpu.SMEM(prompt_len.shape, jnp.int32),
            pltpu.SMEM(suffix_len.shape, jnp.int32),
            pltpu.SMEM(page_table.shape[::-1], jnp.int32),
            vmem((rows, width), bf16),
            pltpu.SMEM((rows,), jnp.int32),
            pltpu.SMEM((rows,), jnp.int32),
            vmem((2, heads, lines, HEAD_SIZE), f32),
            vmem((2, heads, lines, HEAD_SIZE), bf16),
            vmem((2, devices, half, lines, HEAD_SIZE), bf16),
            vmem((2, half, positions, HEAD_SIZE), bf16),
            vmem((2, half, positions, HEAD_SIZE), bf16),
            vmem(suffix_pool_keys.shape, bf16),
            vmem(suffix_pool_values.shape, bf16),
            vmem((2, devices, half, lines, HEAD_SIZE), SENT),
            vmem((2, devices, 2, HEAD_SIZE), f32),
            vmem((2, devices, half, lines, HEAD_SIZE), SENT),
            vmem((2, devices, 2, HEAD_SIZE), f32),
            vmem((devices, half, lines, HEAD_SIZE), f32),
            vmem((heads, 2 * lines, span), bf16),
            vmem((heads, 2, HEAD_SIZE), f32),
            vmem((2, heads, lines, HEAD_SIZE), f32),
            vmem((2, heads, lines, HEAD_SIZE), f32),
            vmem((rows, width), f32),
            dma((5,)),
            dma((2 * half,)),
            dma((2 * half,)),
            dma((2 * half,)),
            dma((2,)),
            dma((devices, 2)),
            dma((devices, 2)),
            dma((devices, 2)),
            dma((devices, 2)),
            dma((devices, 2)),
            dma((devices, 2)),
            pltpu.SemaphoreType.REGULAR((devices // 2,)),
        ],
        compiler_params=pltpu.CompilerParams(
            collective_id=0, has_side_effects=True, vmem_limit_bytes=48 * 1024 * 1024
        ),
    )(
        *(pltpu.with_memory_space_constraint(array, pltpu.HBM) for array in (
            prompt_of.reshape(-1), prompt_len, suffix_len, page_table.T,
            queries, prompt_keys, shared_prompt_values, suffix_pool_keys, suffix_pool_values))
    )


def fits(mesh):
    return mesh.shape["kv"] == 8 and mesh.shape["sub"] == 1


def solution(mesh):
    body = fused if fits(mesh) else shards
    placed = (
        P(("grp", "kv"), "hd"),
        P("grp", None),
        P("grp"),
        P(("grp", "kv")),
        P(("grp", "kv"), "sub"),
        P(("grp", "kv", "sub"), "hd"),
        P(("grp", "kv", "sub"), "hd"),
        P(("grp", "kv", "sub"), None, "hd"),
        P(("grp", "kv", "sub"), None, "hd"),
    )
    return jax.shard_map(
        body, mesh=mesh, in_specs=placed, out_specs=P(("grp", "kv"), "hd"), check_vma=False
    )
```

```python
import functools
import math

import jax
import jax.numpy as jnp
from jax import lax
from jax.experimental import pallas as pl
from jax.experimental.pallas import tpu as pltpu
from jax.sharding import PartitionSpec as P

HEAD_SIZE = 128


NEGATIVE = -1e30


def joined(value, axis, combine):
    everything = jax.tree.map(lambda part: lax.all_gather(part, axis), value)
    leading = jax.tree.map(lambda part: part[0], everything)

    def hop(k, so_far):
        return combine(so_far, jax.tree.map(lambda part: part[k], everything))

    return lax.fori_loop(1, lax.axis_size(axis), hop, leading)


def attend_block(sent_rows, key_block, value_block, lower_bound, upper_bound, first_position):
    row_count = sent_rows.shape[0]
    key_count = key_block.shape[0]
    kv_local = key_block.shape[1] // HEAD_SIZE
    query_group_size = sent_rows.shape[1] // (HEAD_SIZE * kv_local)
    position = first_position + jnp.arange(key_count, dtype=jnp.int32)
    key_mask = (position[None, :] >= lower_bound[:, None]) & (
        position[None, :] < upper_bound[:, None]
    )
    key_mask = key_mask[:, None, :]
    score_scale = 1.0 / math.sqrt(HEAD_SIZE)
    blended_parts = []
    lse_parts = []
    for kv_head in range(kv_local):
        low_column = kv_head * query_group_size * HEAD_SIZE
        head_query = sent_rows[:, low_column : low_column + query_group_size * HEAD_SIZE].reshape(
            row_count * query_group_size, HEAD_SIZE
        )
        head_keys = key_block[:, kv_head * HEAD_SIZE : (kv_head + 1) * HEAD_SIZE]
        head_values = value_block[:, kv_head * HEAD_SIZE : (kv_head + 1) * HEAD_SIZE]
        scores = lax.dot_general(
            head_query, head_keys, (((1,), (1,)), ((), ())), preferred_element_type=jnp.float32
        )
        scores = (scores * score_scale).reshape(row_count, query_group_size, key_count)
        scores = jnp.where(key_mask, scores, NEGATIVE)
        row_max = jnp.max(scores, axis=2, keepdims=True)
        weights = jnp.where(key_mask, jnp.exp(scores - row_max), 0.0)
        totals = jnp.maximum(jnp.sum(weights, axis=2), 1.0)
        weighted = jnp.dot(
            weights.astype(jnp.bfloat16).reshape(row_count * query_group_size, key_count),
            head_values,
            preferred_element_type=jnp.float32,
        )
        weighted = weighted.reshape(row_count, query_group_size, HEAD_SIZE) / totals[:, :, None]
        blended_parts.append(weighted.reshape(row_count, query_group_size * HEAD_SIZE))
        lse_parts.append(row_max[:, :, 0] + jnp.log(totals))
    return (jnp.concatenate(blended_parts, axis=1), jnp.concatenate(lse_parts, axis=1))


def combine_halves(earlier, later):
    joint_max = jnp.maximum(earlier[0], later[0])
    left_factor = jnp.exp(earlier[0] - joint_max)
    right_factor = jnp.exp(later[0] - joint_max)
    totals = earlier[1] * left_factor + later[1] * right_factor
    blended = earlier[2] * left_factor[:, :, None] + later[2] * right_factor[:, :, None]
    return (joint_max, totals, blended)


def shards(
    queries,
    prompt_of,
    prompt_len,
    suffix_len,
    page_table,
    prompt_keys,
    shared_prompt_values,
    suffix_pool_keys,
    suffix_pool_values,
):
    kv_count = lax.axis_size("kv")
    sub_count = lax.axis_size("sub")
    kv_index = lax.axis_index("kv")
    sub_index = lax.axis_index("sub")
    seq_local = queries.shape[0]
    row_width = queries.shape[1]
    heads_local = row_width // HEAD_SIZE
    cache_local = prompt_keys.shape[0]
    kv_reach = sub_count * cache_local
    prompt_count = prompt_len.shape[0]
    prompt_starts = jnp.cumsum(prompt_len) - prompt_len
    prompt_ends = prompt_starts + prompt_len
    prompt_labels = jnp.arange(prompt_count, dtype=jnp.int32)
    range_low = jnp.arange(kv_count, dtype=jnp.int32) * kv_reach
    intersections = (prompt_starts[None, :] < range_low[:, None] + kv_reach) & (
        prompt_ends[None, :] > range_low[:, None]
    )
    later_slot = prompt_starts[None, :] > range_low[:, None]
    first_position = (kv_index * sub_count + sub_index) * cache_local
    most_rows = seq_local // prompt_count
    owned_prompt = lax.dynamic_slice_in_dim(prompt_of[:, 0], kv_index * seq_local, seq_local)
    prompt_hits = owned_prompt[:, None] == prompt_labels[None, :]
    hit_counts = prompt_hits.astype(jnp.int32)
    ranks = jnp.sum((jnp.cumsum(hit_counts, axis=0) - hit_counts) * hit_counts, axis=1)
    seq_intersection = jnp.any(intersections[:, None, :] & prompt_hits[None, :, :], axis=2)
    seq_later = jnp.any(later_slot[:, None, :] & prompt_hits[None, :, :], axis=2).astype(jnp.int32)
    slot_labels = jnp.arange(2, dtype=jnp.int32)
    rank_labels = jnp.arange(most_rows, dtype=jnp.int32)
    selector = seq_intersection[:, None, None, :] & (
        seq_later[:, None, None, :] == slot_labels[None, :, None, None]
    )
    selector = selector & (ranks[None, None, None, :] == rank_labels[None, None, :, None])
    selector = selector.reshape(kv_count * 2 * most_rows, seq_local)
    outgoing = jnp.dot(
        selector.astype(jnp.bfloat16), queries, preferred_element_type=jnp.float32
    ).astype(jnp.bfloat16)
    incoming = lax.all_to_all(
        outgoing.reshape(kv_count, 2 * most_rows, row_width),
        "kv",
        split_axis=0,
        concat_axis=0,
        tiled=True,
    )
    mine_intersection = lax.dynamic_index_in_dim(intersections, kv_index, 0, keepdims=False)
    mine_later = lax.dynamic_index_in_dim(later_slot, kv_index, 0, keepdims=False).astype(jnp.int32)
    chosen = mine_intersection[None, :] & (mine_later[None, :] == slot_labels[:, None])
    slot_low = jnp.sum(jnp.where(chosen, prompt_starts[None, :], 0), axis=1)
    slot_high = jnp.sum(jnp.where(chosen, prompt_ends[None, :], 0), axis=1)
    lower_bound = jnp.broadcast_to(
        jnp.repeat(slot_low, most_rows)[None, :], (kv_count, 2 * most_rows)
    ).reshape(-1)
    upper_bound = jnp.broadcast_to(
        jnp.repeat(slot_high, most_rows)[None, :], (kv_count, 2 * most_rows)
    ).reshape(-1)
    sent_rows = incoming.reshape(kv_count * 2 * most_rows, row_width)
    back_rows = 2 * most_rows
    prompt_out, prompt_lse = attend_block(
        sent_rows, prompt_keys, shared_prompt_values, lower_bound, upper_bound, first_position
    )
    returned_out, returned_lse = (
        lax.all_to_all(
            prompt_out.reshape(kv_count, back_rows, row_width),
            "kv",
            split_axis=0,
            concat_axis=0,
            tiled=True,
        ),
        lax.all_to_all(
            prompt_lse.reshape(kv_count, back_rows, heads_local),
            "kv",
            split_axis=0,
            concat_axis=0,
            tiled=True,
        ),
    )
    page_slots = page_table.shape[1]
    page_length = suffix_pool_keys.shape[1]
    suffix_span = page_slots * page_length
    gathered_keys = suffix_pool_keys[page_table].reshape(seq_local, suffix_span, -1)
    gathered_values = suffix_pool_values[page_table].reshape(seq_local, suffix_span, -1)
    suffix_first = sub_index * suffix_span

    def one_sequence(query_line, seq_keys, seq_values, seq_length):
        return attend_block(
            query_line[None, :],
            seq_keys,
            seq_values,
            jnp.zeros((1,), jnp.int32),
            seq_length[None],
            suffix_first,
        )

    suffix_out, suffix_lse = jax.vmap(one_sequence)(
        queries, gathered_keys, gathered_values, suffix_len
    )
    suffix_out = suffix_out[:, 0].reshape(seq_local, heads_local, HEAD_SIZE)
    suffix_lse = suffix_lse[:, 0]
    flat_lse = returned_lse.reshape(-1, heads_local)
    flat_out = returned_out.reshape(-1, heads_local, HEAD_SIZE)
    masked_lse = jnp.where(selector[:, :, None], flat_lse[:, None, :], NEGATIVE)
    joint_max = jnp.maximum(jnp.max(masked_lse, axis=0), suffix_lse)
    factors = jnp.where(selector[:, :, None], jnp.exp(masked_lse - joint_max[None]), 0.0)
    own_factor = jnp.exp(suffix_lse - joint_max)
    totals = jnp.sum(factors, axis=0) + own_factor
    blended = jnp.einsum("rsh,rhd->shd", factors, flat_out, precision=lax.Precision.HIGHEST)
    blended = blended + own_factor[:, :, None] * suffix_out
    joint_max, totals, blended = joined((joint_max, totals, blended), "sub", combine_halves)
    return (blended / totals[:, :, None]).reshape(seq_local, row_width).astype(jnp.float32)


SENT = jnp.int16
STEPS = 32000.0
TINY = 1e-30
LOG2E = 1.4426950408889634
FIRST_SLOT = (0, 0, 1, 1)
HOLDERS = (((0, 0), (1, 0)), ((1, 1), (2, 0), (3, 0)))
CHUNK = 4
SENDS = ((2, 0), (3, 0), (0, 0), (1, 0), (2, 1), (3, 1), (4, 0), (5, 0), (6, 0), (7, 0))


def windows(chip):
    return (0, 1) if chip == 1 else (FIRST_SLOT[chip],)


def lanes(column, width=HEAD_SIZE):
    return jnp.broadcast_to(column, (column.shape[0], width))


def standing(row):
    return jnp.broadcast_to(row, (HEAD_SIZE, HEAD_SIZE)).T


def attend(
    of_ref, len_ref, suf_ref, table_ref, q_in, pk_ref, pv_ref, sk_ref, sv_ref,
    out_ref,
    prompt_of, prompt_len, suffix_len, page_table, q_ref, order, places, qf, q_send, q_all, kbuf, vbuf, pool_k, pool_v,
    o_send, l_send, o_recv, l_recv, l_cols, suf_w, suf_s, suf_o, suf_l, merged,
    in_sem, own_sem, swap_send, swap_recv, pool_sem, qs_sem, qr_sem, os_sem, or_sem, ls_sem, lr_sem,
    relay_sem, ready_sem, held, held_top,
):
    me = lax.axis_index("kv")
    chip = me // 2
    core = me % 2
    other = 1 - core
    partner = chip * 2 + other
    devices = 8
    rows = q_ref.shape[0]
    most = rows // 2
    heads = pk_ref.shape[1] // HEAD_SIZE
    half = heads // 2
    group = q_ref.shape[1] // (heads * HEAD_SIZE)
    positions = pk_ref.shape[0]
    lines = group * most
    slots = page_table.shape[0]
    span = slots * sk_ref.shape[1]
    scale = LOG2E / math.sqrt(HEAD_SIZE)

    def columns(head):
        return pl.ds(pl.multiple_of(head * HEAD_SIZE, HEAD_SIZE), HEAD_SIZE)

    def signal(semaphore, dst):
        pl.semaphore_signal(semaphore, inc=1, device_id={"kv": dst},
                            device_id_type=pl.DeviceIdType.MESH)

    barrier = pltpu.get_barrier_semaphore()
    for dst in range(devices):
        @pl.when((dst == partner) | (dst // 2 > chip))
        def _():
            signal(barrier, dst)

    pool_copies = [pltpu.make_async_copy(sk_ref, pool_k, pool_sem.at[0]),
                   pltpu.make_async_copy(sv_ref, pool_v, pool_sem.at[1])]
    own_copies = []
    for h in range(half):
        for i, (ref, buf) in enumerate(((pk_ref, kbuf), (pv_ref, vbuf))):
            own_copies.append(pltpu.make_async_copy(
                ref.at[:, columns(core * half + h)], buf.at[core, h], own_sem.at[2 * h + i]))
    inputs = [pltpu.make_async_copy(src, dst, in_sem.at[i]) for i, (src, dst) in enumerate((
        (of_ref, prompt_of), (len_ref, prompt_len), (suf_ref, suffix_len),
        (table_ref, page_table), (q_in, q_ref)))]
    for copy in inputs:
        copy.start()
    pool_copies[0].start()
    for copy in own_copies:
        copy.start()
    pl.semaphore_wait(barrier, 2 * chip + 1)
    for dst in range(devices):
        @pl.when(dst // 2 < chip)
        def _():
            signal(ready_sem.at[chip], dst)

    def swap_copies():
        made = []
        for h in range(half):
            for i, (ref, buf) in enumerate(((pk_ref, kbuf), (pv_ref, vbuf))):
                made.append(pltpu.make_async_remote_copy(
                    src_ref=ref.at[:, columns(other * half + h)], dst_ref=buf.at[core, h],
                    send_sem=swap_send.at[2 * h + i], recv_sem=swap_recv.at[2 * h + i],
                    device_id={"kv": partner}, device_id_type=pl.DeviceIdType.MESH))
        return made

    swaps = swap_copies()
    for copy in swaps:
        copy.start()

    for copy in inputs:
        copy.wait()

    count = [jnp.int32(0), jnp.int32(0)]
    place = []
    for s in range(rows):
        is_one = prompt_of[me * rows + s]
        place.append(jnp.where(is_one == 1, most + count[1], count[0]))
        count[0] = count[0] + (1 - is_one)
        count[1] = count[1] + is_one
        places[s] = place[s]
    row_ids = lax.broadcasted_iota(jnp.int32, (rows, rows), 0)
    col_ids = lax.broadcasted_iota(jnp.int32, (rows, rows), 1)
    chooser = jnp.zeros((rows, rows), jnp.float32)
    for s in range(rows):
        chooser = jnp.where((row_ids == place[s]) & (col_ids == s), 1.0, chooser)
    for r in range(rows):
        found = jnp.int32(0)
        for s in range(rows):
            found = jnp.where(place[s] == r, s, found)
        order[r] = found
    chooser = chooser.astype(jnp.bfloat16)

    for h in range(heads):
        width = group * HEAD_SIZE
        block = jnp.dot(chooser, q_ref[:, h * width:(h + 1) * width],
                        preferred_element_type=jnp.float32)
        for p in range(2):
            tall = jnp.concatenate(
                [block[p * most:(p + 1) * most, g * HEAD_SIZE:(g + 1) * HEAD_SIZE]
                 for g in range(group)], axis=0)
            qf[p, h] = tall
            q_send[p, h] = tall.astype(jnp.bfloat16)

    def query_copy(dst, slot, src):
        prompt = windows(dst // 2)[slot]
        return pltpu.make_async_remote_copy(
            src_ref=q_send.at[prompt, pl.ds(dst % 2 * half, half)], dst_ref=q_all.at[slot, src],
            send_sem=qs_sem.at[dst, slot], recv_sem=qr_sem.at[src, slot],
            device_id={"kv": dst}, device_id_type=pl.DeviceIdType.MESH)

    def send_up(to):
        pl.semaphore_wait(ready_sem.at[to], 2)
        for dst, slot in SENDS:
            if dst // 2 == to:
                query_copy(dst, slot, me).start()

    for dst, slot in SENDS:
        @pl.when((me != dst) & (dst // 2 <= chip) & ((chip < 2) | ((slot == 0) & (dst > 1))))
        def _():
            query_copy(dst, slot, me).start()

        @pl.when(me == dst)
        def _():
            q_all[slot, me] = q_send[windows(dst // 2)[slot], (dst % 2) * half:(dst % 2 + 1) * half]

    @pl.when(chip == 0)
    def _():
        send_up(1)

    @pl.when(chip == 1)
    def _():
        send_up(2)

    @pl.when((chip == 1) | (chip == 2))
    def _():
        send_up(3)

    spots = lax.broadcasted_iota(jnp.int32, (span, HEAD_SIZE), 0)
    lane = lax.broadcasted_iota(jnp.int32, (1, HEAD_SIZE), 1)
    pairs = heads // 2

    def gathered(pool, s, columns_of):
        return jnp.concatenate(
            [pool[page_table[j, s], :, columns_of] for j in range(slots)], axis=0)

    pool_copies[0].wait()
    pool_copies[1].start()

    @pl.when(chip >= 2)
    def _():
        for dst, slot in SENDS:
            if slot == 1:
                query_copy(dst, slot, me).start()

    def suffix_scores(batch):
        p, pair = batch // pairs, batch % pairs
        wanted = pl.ds(pl.multiple_of(pair * 2 * HEAD_SIZE, 2 * HEAD_SIZE), 2 * HEAD_SIZE)
        tall = qf[p, pl.ds(pair * 2, 2)].reshape(2 * lines, HEAD_SIZE).T.astype(jnp.bfloat16)
        scores = None
        length = jnp.zeros((1, HEAD_SIZE), jnp.int32)
        for rank in range(most):
            s = order[p * most + rank]
            mine = lane % most == rank
            length = jnp.where(mine, suffix_len[s], length)
            both = [jnp.where(mine & (lane // lines == i), 1.0, 0.0).astype(jnp.bfloat16)
                    for i in range(2)]
            query = jnp.concatenate([tall * both[0], tall * both[1]], axis=0)
            part = jnp.dot(gathered(pool_k, s, wanted), query, preferred_element_type=jnp.float32)
            scores = part if scores is None else scores + part
        scores = jnp.where(spots < length, scores * scale, NEGATIVE)
        top = jnp.max(scores, axis=0, keepdims=True)
        weights = jnp.exp2(scores - top)
        total = jnp.sum(weights, axis=0, keepdims=True)
        suf_w[batch] = weights.T.astype(jnp.bfloat16)
        suf_s[batch, 0:1] = top + jnp.log2(total)
        suf_s[batch, 1:2] = 1.0 / total

    def suffix_half(p):
        for pair in range(pairs):
            suffix_scores(p * pairs + pair)

    @pl.loop(0, jnp.where(chip == 1, 1, 2))
    def _(p):
        suffix_half(p)

        @pl.when((chip == 0) & (p == 0))
        def _():
            for to in (2, 3):
                send_up(to)

    for copy in own_copies:
        copy.wait()
    for copy in swaps:
        copy.wait_recv()

    first_end = prompt_len[0]
    second_end = first_end + prompt_len[1]

    def wait_query(src, slot):
        pltpu.make_async_remote_copy(
            src_ref=q_send.at[0, pl.ds(0, half)], dst_ref=q_all.at[slot, src],
            send_sem=qs_sem.at[src, slot], recv_sem=qr_sem.at[src, slot],
            device_id={"kv": src}, device_id_type=pl.DeviceIdType.MESH).wait_recv()

    def relay_copy(offset):
        src = CHUNK + offset
        return pltpu.make_async_remote_copy(
            src_ref=q_all.at[0, src], dst_ref=q_all.at[0, src],
            send_sem=relay_sem.at[offset], recv_sem=qr_sem.at[src, 0],
            device_id={"kv": core}, device_id_type=pl.DeviceIdType.MESH)

    def head_copy(dst, slot, sender, h):
        return pltpu.make_async_remote_copy(
            src_ref=o_send.at[slot, dst, h], dst_ref=o_recv.at[slot, sender, h],
            send_sem=os_sem.at[dst, slot, h], recv_sem=or_sem.at[sender, slot, h],
            device_id={"kv": dst}, device_id_type=pl.DeviceIdType.MESH)

    def facts_copy(dst, slot, sender):
        return pltpu.make_async_remote_copy(
            src_ref=l_send.at[slot, dst], dst_ref=l_recv.at[slot, sender],
            send_sem=ls_sem.at[dst, slot], recv_sem=lr_sem.at[sender, slot],
            device_id={"kv": dst}, device_id_type=pl.DeviceIdType.MESH)

    def back_copies(dst, slot, sender):
        return [head_copy(dst, slot, sender, h) for h in range(half)] + [facts_copy(dst, slot, sender)]

    is_level = lax.broadcasted_iota(jnp.int32, (CHUNK * lines, HEAD_SIZE), 1) % 2 == 0

    def prompt_turn(slot, turn, low, high, first_block):
        blocks = 2 - first_block
        spot = (chip * 2 + first_block) * positions + lax.broadcasted_iota(
            jnp.int32, (1, blocks * positions), 1)
        bias = jnp.where((spot >= low) & (spot < high), 0.0, NEGATIVE)
        begin = turn * CHUNK

        @pl.loop(0, CHUNK)
        def _(offset):
            src = begin + offset

            @pl.when((me != src) & ((chip != 1) | (turn == 0) | (slot == 1)))
            def _():
                wait_query(src, slot)

        width = blocks * positions

        def scored(h):
            query = q_all[slot, pl.ds(begin, CHUNK), h].reshape(CHUNK * lines, HEAD_SIZE)
            keys = kbuf[first_block:2, h].reshape(width, HEAD_SIZE)
            scores = lax.dot_general(query, keys, (((1,), (1,)), ((), ())),
                                     preferred_element_type=jnp.float32)
            scores = scores * scale + bias
            return scores, lanes(jnp.max(scores, axis=1, keepdims=True))

        def finished(h, scores, top):
            values = vbuf[first_block:2, h].reshape(width, HEAD_SIZE)
            weights = jnp.exp2(scores - jnp.concatenate([top] * (width // HEAD_SIZE), axis=1))
            total = jnp.sum(weights, axis=1, keepdims=True)
            mixed = jnp.dot(weights.astype(jnp.bfloat16), values,
                            preferred_element_type=jnp.float32)
            peak = jnp.maximum(jnp.max(jnp.abs(mixed), axis=1, keepdims=True), TINY)
            steps = jnp.round(mixed * (STEPS / peak)).astype(jnp.int32)
            o_send[slot, pl.ds(begin, CHUNK), h] = steps.astype(SENT).reshape(
                CHUNK, lines, HEAD_SIZE)
            peak = peak * (1.0 / (STEPS * total))
            facts = jnp.where(is_level, top + lanes(jnp.log2(total)), lanes(peak))
            l_cols[pl.ds(begin, CHUNK), h] = facts.reshape(CHUNK, lines, HEAD_SIZE)

        def returned(h):
            @pl.loop(0, CHUNK)
            def _(offset):
                @pl.when(me != begin + offset)
                def _():
                    head_copy(begin + offset, slot, me, h).start()

        ready = scored(0)
        for h in range(half):
            finished(h, *ready)
            if h + 1 < half:
                scores, top = scored(h + 1)
                held[:, :width] = scores
                held_top[...] = top
            if slot == 1 and h == 0:
                @pl.when(turn == 0)
                def _():
                    for i in range(CHUNK):
                        wait_query(CHUNK + i, 0)
                        relay_copy(i).start()
            returned(h)
            if h + 1 < half:
                ready = (held[:, :width], held_top[...])

        @pl.loop(0, CHUNK)
        def _(offset):
            dst = begin + offset
            turned = l_cols[dst].reshape(half * lines, HEAD_SIZE).T
            l_send[slot, dst] = turned[0:2]

            @pl.when(me != dst)
            def _():
                facts_copy(dst, slot, me).start()

            @pl.when(me == dst)
            def _():
                o_recv[slot, me] = o_send[slot, dst]
                l_recv[slot, me] = l_send[slot, dst]

    low, high = jnp.where(chip < 2, 0, first_end), jnp.where(chip < 2, first_end, second_end)
    row = lax.broadcasted_iota(jnp.int32, (2 * lines, HEAD_SIZE), 0)

    def suffix_values():
        pool_copies[1].wait()

        @pl.loop(0, 2 * pairs)
        def _(batch):
            p, pair = batch // pairs, batch % pairs
            wanted = pl.ds(pl.multiple_of(pair * 2 * HEAD_SIZE, 2 * HEAD_SIZE), 2 * HEAD_SIZE)
            weights = suf_w[batch]
            mixed = None
            for rank in range(most):
                s = order[p * most + rank]
                mine = jnp.where(row % most == rank, 1.0, 0.0).astype(jnp.bfloat16)
                mine = jnp.concatenate([mine] * (span // HEAD_SIZE), axis=1)
                part = jnp.dot(weights * mine, gathered(pool_v, s, wanted),
                               preferred_element_type=jnp.float32)
                mixed = part if mixed is None else mixed + part
            level, inverse = standing(suf_s[batch, 0:1]), standing(suf_s[batch, 1:2])
            for i in range(2):
                mine = slice(i * lines, (i + 1) * lines)
                suf_o[p, pair * 2 + i] = (
                    mixed[mine, i * HEAD_SIZE:(i + 1) * HEAD_SIZE] * inverse[mine])
                suf_l[p, pair * 2 + i] = level[mine]

    @pl.loop(0, 2)
    def _(step):
        @pl.when(chip == 1)
        def _():
            prompt_turn(1, step, first_end, second_end, 1)

        prompt_turn(0, jnp.where(chip == 1, 1 - step, step), low, high, 0)

        @pl.when((chip == 1) & (step == 1))
        def _():
            suffix_half(1)

        @pl.when(step == jnp.where(chip == 1, 1, 0))
        def _():
            suffix_values()

    for p in range(2):
        for d in range(2):
            arrived, levels = [], []
            for c, slot in HOLDERS[p]:
                sender = 2 * c + d

                @pl.when(me != sender)
                def _():
                    for copy in back_copies(sender, slot, sender):
                        copy.wait_recv()

                levels.append((standing(l_recv[slot, sender, 0:1]), standing(l_recv[slot, sender, 1:2])))
                arrived.append((slot, sender))
            for hh in range(half):
                h = d * half + hh
                mine = slice(hh * lines, (hh + 1) * lines)
                parts = [(level[mine], o_recv[slot, sender, hh].astype(jnp.int32).astype(jnp.float32)
                          * step[mine])
                         for (level, step), (slot, sender) in zip(levels, arrived)]
                parts.append((suf_l[p, h], suf_o[p, h]))
                joint = functools.reduce(jnp.maximum, [level for level, _ in parts])
                factors = [jnp.exp2(level - joint) for level, _ in parts]
                total = functools.reduce(jnp.add, factors)
                blend = functools.reduce(jnp.add, [f * o for f, (_, o) in zip(factors, parts)])
                blend = blend / total
                for g in range(group):
                    first = (h * group + g) * HEAD_SIZE
                    merged[p * most:(p + 1) * most, first:first + HEAD_SIZE] = (
                        blend[g * most:(g + 1) * most])

    for s in range(rows):
        out_ref[s:s + 1, :] = merged[pl.ds(places[s], 1), :]

    for copy in swaps:
        copy.wait_send()

    for dst, slot in SENDS:
        @pl.when((me != dst) & ((chip < 2) | (dst > 1)))
        def _():
            query_copy(dst, slot, me).wait_send()

    @pl.when(chip == 1)
    def _():
        for i in range(CHUNK):
            relay_copy(i).wait_send()

    for dst in range(devices):
        @pl.when(me != dst)
        def _():
            for copy in back_copies(dst, 0, me):
                copy.wait_send()

        @pl.when((me != dst) & (chip == 1))
        def _():
            for copy in back_copies(dst, 1, me):
                copy.wait_send()


def fused(
    queries,
    prompt_of,
    prompt_len,
    suffix_len,
    page_table,
    prompt_keys,
    shared_prompt_values,
    suffix_pool_keys,
    suffix_pool_values,
):
    rows, width = queries.shape
    most = rows // 2
    positions, depth = prompt_keys.shape
    heads = depth // HEAD_SIZE
    half = heads // 2
    group = width // depth
    lines = group * most
    span = page_table.shape[1] * suffix_pool_keys.shape[1]
    devices = lax.axis_size("kv")
    f32, bf16 = jnp.float32, jnp.bfloat16
    vmem, dma = pltpu.VMEM, pltpu.SemaphoreType.DMA
    return pl.pallas_call(
        attend,
        out_shape=pltpu.VMEM((rows, width), f32),
        in_specs=[pl.BlockSpec(memory_space=pl.ANY)] * 9,
        out_specs=pl.BlockSpec(memory_space=pltpu.VMEM),
        scratch_shapes=[
            pltpu.SMEM(prompt_of.shape[:1], jnp.int32),
            pltpu.SMEM(prompt_len.shape, jnp.int32),
            pltpu.SMEM(suffix_len.shape, jnp.int32),
            pltpu.SMEM(page_table.shape[::-1], jnp.int32),
            vmem((rows, width), bf16),
            pltpu.SMEM((rows,), jnp.int32),
            pltpu.SMEM((rows,), jnp.int32),
            vmem((2, heads, lines, HEAD_SIZE), f32),
            vmem((2, heads, lines, HEAD_SIZE), bf16),
            vmem((2, devices, half, lines, HEAD_SIZE), bf16),
            vmem((2, half, positions, HEAD_SIZE), bf16),
            vmem((2, half, positions, HEAD_SIZE), bf16),
            vmem(suffix_pool_keys.shape, bf16),
            vmem(suffix_pool_values.shape, bf16),
            vmem((2, devices, half, lines, HEAD_SIZE), SENT),
            vmem((2, devices, 2, HEAD_SIZE), f32),
            vmem((2, devices, half, lines, HEAD_SIZE), SENT),
            vmem((2, devices, 2, HEAD_SIZE), f32),
            vmem((devices, half, lines, HEAD_SIZE), f32),
            vmem((heads, 2 * lines, span), bf16),
            vmem((heads, 2, HEAD_SIZE), f32),
            vmem((2, heads, lines, HEAD_SIZE), f32),
            vmem((2, heads, lines, HEAD_SIZE), f32),
            vmem((rows, width), f32),
            dma((5,)),
            dma((2 * half,)),
            dma((2 * half,)),
            dma((2 * half,)),
            dma((2,)),
            dma((devices, 2)),
            dma((devices, 2)),
            dma((devices, 2, half)),
            dma((devices, 2, half)),
            dma((devices, 2)),
            dma((devices, 2)),
            dma((CHUNK,)),
            pltpu.SemaphoreType.REGULAR((devices // 2,)),
            vmem((CHUNK * lines, 2 * positions), f32),
            vmem((CHUNK * lines, HEAD_SIZE), f32),
        ],
        compiler_params=pltpu.CompilerParams(
            collective_id=0, has_side_effects=True, vmem_limit_bytes=48 * 1024 * 1024
        ),
    )(
        *(pltpu.with_memory_space_constraint(array, pltpu.HBM) for array in (
            prompt_of.reshape(-1), prompt_len, suffix_len, page_table.T,
            queries, prompt_keys, shared_prompt_values, suffix_pool_keys, suffix_pool_values))
    )


def fits(mesh):
    return mesh.shape["kv"] == 8 and mesh.shape["sub"] == 1


def solution(mesh):
    body = fused if fits(mesh) else shards
    placed = (
        P(("grp", "kv"), "hd"),
        P("grp", None),
        P("grp"),
        P(("grp", "kv")),
        P(("grp", "kv"), "sub"),
        P(("grp", "kv", "sub"), "hd"),
        P(("grp", "kv", "sub"), "hd"),
        P(("grp", "kv", "sub"), None, "hd"),
        P(("grp", "kv", "sub"), None, "hd"),
    )
    return jax.shard_map(
        body, mesh=mesh, in_specs=placed, out_specs=P(("grp", "kv"), "hd"), check_vma=False
    )
```

```python
import functools
import math

import jax
import jax.numpy as jnp
from jax import lax
from jax.experimental import pallas as pl
from jax.experimental.pallas import tpu as pltpu
from jax.sharding import PartitionSpec as P

HEAD_SIZE = 128


NEGATIVE = -1e30


def joined(value, axis, combine):
    everything = jax.tree.map(lambda part: lax.all_gather(part, axis), value)
    leading = jax.tree.map(lambda part: part[0], everything)

    def hop(k, so_far):
        return combine(so_far, jax.tree.map(lambda part: part[k], everything))

    return lax.fori_loop(1, lax.axis_size(axis), hop, leading)


def attend_block(sent_rows, key_block, value_block, lower_bound, upper_bound, first_position):
    row_count = sent_rows.shape[0]
    key_count = key_block.shape[0]
    kv_local = key_block.shape[1] // HEAD_SIZE
    query_group_size = sent_rows.shape[1] // (HEAD_SIZE * kv_local)
    position = first_position + jnp.arange(key_count, dtype=jnp.int32)
    key_mask = (position[None, :] >= lower_bound[:, None]) & (
        position[None, :] < upper_bound[:, None]
    )
    key_mask = key_mask[:, None, :]
    score_scale = 1.0 / math.sqrt(HEAD_SIZE)
    blended_parts = []
    lse_parts = []
    for kv_head in range(kv_local):
        low_column = kv_head * query_group_size * HEAD_SIZE
        head_query = sent_rows[:, low_column : low_column + query_group_size * HEAD_SIZE].reshape(
            row_count * query_group_size, HEAD_SIZE
        )
        head_keys = key_block[:, kv_head * HEAD_SIZE : (kv_head + 1) * HEAD_SIZE]
        head_values = value_block[:, kv_head * HEAD_SIZE : (kv_head + 1) * HEAD_SIZE]
        scores = lax.dot_general(
            head_query, head_keys, (((1,), (1,)), ((), ())), preferred_element_type=jnp.float32
        )
        scores = (scores * score_scale).reshape(row_count, query_group_size, key_count)
        scores = jnp.where(key_mask, scores, NEGATIVE)
        row_max = jnp.max(scores, axis=2, keepdims=True)
        weights = jnp.where(key_mask, jnp.exp(scores - row_max), 0.0)
        totals = jnp.maximum(jnp.sum(weights, axis=2), 1.0)
        weighted = jnp.dot(
            weights.astype(jnp.bfloat16).reshape(row_count * query_group_size, key_count),
            head_values,
            preferred_element_type=jnp.float32,
        )
        weighted = weighted.reshape(row_count, query_group_size, HEAD_SIZE) / totals[:, :, None]
        blended_parts.append(weighted.reshape(row_count, query_group_size * HEAD_SIZE))
        lse_parts.append(row_max[:, :, 0] + jnp.log(totals))
    return (jnp.concatenate(blended_parts, axis=1), jnp.concatenate(lse_parts, axis=1))


def combine_halves(earlier, later):
    joint_max = jnp.maximum(earlier[0], later[0])
    left_factor = jnp.exp(earlier[0] - joint_max)
    right_factor = jnp.exp(later[0] - joint_max)
    totals = earlier[1] * left_factor + later[1] * right_factor
    blended = earlier[2] * left_factor[:, :, None] + later[2] * right_factor[:, :, None]
    return (joint_max, totals, blended)


def shards(
    queries,
    prompt_of,
    prompt_len,
    suffix_len,
    page_table,
    prompt_keys,
    shared_prompt_values,
    suffix_pool_keys,
    suffix_pool_values,
):
    kv_count = lax.axis_size("kv")
    sub_count = lax.axis_size("sub")
    kv_index = lax.axis_index("kv")
    sub_index = lax.axis_index("sub")
    seq_local = queries.shape[0]
    row_width = queries.shape[1]
    heads_local = row_width // HEAD_SIZE
    cache_local = prompt_keys.shape[0]
    kv_reach = sub_count * cache_local
    prompt_count = prompt_len.shape[0]
    prompt_starts = jnp.cumsum(prompt_len) - prompt_len
    prompt_ends = prompt_starts + prompt_len
    prompt_labels = jnp.arange(prompt_count, dtype=jnp.int32)
    range_low = jnp.arange(kv_count, dtype=jnp.int32) * kv_reach
    intersections = (prompt_starts[None, :] < range_low[:, None] + kv_reach) & (
        prompt_ends[None, :] > range_low[:, None]
    )
    later_slot = prompt_starts[None, :] > range_low[:, None]
    first_position = (kv_index * sub_count + sub_index) * cache_local
    most_rows = seq_local // prompt_count
    owned_prompt = lax.dynamic_slice_in_dim(prompt_of[:, 0], kv_index * seq_local, seq_local)
    prompt_hits = owned_prompt[:, None] == prompt_labels[None, :]
    hit_counts = prompt_hits.astype(jnp.int32)
    ranks = jnp.sum((jnp.cumsum(hit_counts, axis=0) - hit_counts) * hit_counts, axis=1)
    seq_intersection = jnp.any(intersections[:, None, :] & prompt_hits[None, :, :], axis=2)
    seq_later = jnp.any(later_slot[:, None, :] & prompt_hits[None, :, :], axis=2).astype(jnp.int32)
    slot_labels = jnp.arange(2, dtype=jnp.int32)
    rank_labels = jnp.arange(most_rows, dtype=jnp.int32)
    selector = seq_intersection[:, None, None, :] & (
        seq_later[:, None, None, :] == slot_labels[None, :, None, None]
    )
    selector = selector & (ranks[None, None, None, :] == rank_labels[None, None, :, None])
    selector = selector.reshape(kv_count * 2 * most_rows, seq_local)
    outgoing = jnp.dot(
        selector.astype(jnp.bfloat16), queries, preferred_element_type=jnp.float32
    ).astype(jnp.bfloat16)
    incoming = lax.all_to_all(
        outgoing.reshape(kv_count, 2 * most_rows, row_width),
        "kv",
        split_axis=0,
        concat_axis=0,
        tiled=True,
    )
    mine_intersection = lax.dynamic_index_in_dim(intersections, kv_index, 0, keepdims=False)
    mine_later = lax.dynamic_index_in_dim(later_slot, kv_index, 0, keepdims=False).astype(jnp.int32)
    chosen = mine_intersection[None, :] & (mine_later[None, :] == slot_labels[:, None])
    slot_low = jnp.sum(jnp.where(chosen, prompt_starts[None, :], 0), axis=1)
    slot_high = jnp.sum(jnp.where(chosen, prompt_ends[None, :], 0), axis=1)
    lower_bound = jnp.broadcast_to(
        jnp.repeat(slot_low, most_rows)[None, :], (kv_count, 2 * most_rows)
    ).reshape(-1)
    upper_bound = jnp.broadcast_to(
        jnp.repeat(slot_high, most_rows)[None, :], (kv_count, 2 * most_rows)
    ).reshape(-1)
    sent_rows = incoming.reshape(kv_count * 2 * most_rows, row_width)
    back_rows = 2 * most_rows
    prompt_out, prompt_lse = attend_block(
        sent_rows, prompt_keys, shared_prompt_values, lower_bound, upper_bound, first_position
    )
    returned_out, returned_lse = (
        lax.all_to_all(
            prompt_out.reshape(kv_count, back_rows, row_width),
            "kv",
            split_axis=0,
            concat_axis=0,
            tiled=True,
        ),
        lax.all_to_all(
            prompt_lse.reshape(kv_count, back_rows, heads_local),
            "kv",
            split_axis=0,
            concat_axis=0,
            tiled=True,
        ),
    )
    page_slots = page_table.shape[1]
    page_length = suffix_pool_keys.shape[1]
    suffix_span = page_slots * page_length
    gathered_keys = suffix_pool_keys[page_table].reshape(seq_local, suffix_span, -1)
    gathered_values = suffix_pool_values[page_table].reshape(seq_local, suffix_span, -1)
    suffix_first = sub_index * suffix_span

    def one_sequence(query_line, seq_keys, seq_values, seq_length):
        return attend_block(
            query_line[None, :],
            seq_keys,
            seq_values,
            jnp.zeros((1,), jnp.int32),
            seq_length[None],
            suffix_first,
        )

    suffix_out, suffix_lse = jax.vmap(one_sequence)(
        queries, gathered_keys, gathered_values, suffix_len
    )
    suffix_out = suffix_out[:, 0].reshape(seq_local, heads_local, HEAD_SIZE)
    suffix_lse = suffix_lse[:, 0]
    flat_lse = returned_lse.reshape(-1, heads_local)
    flat_out = returned_out.reshape(-1, heads_local, HEAD_SIZE)
    masked_lse = jnp.where(selector[:, :, None], flat_lse[:, None, :], NEGATIVE)
    joint_max = jnp.maximum(jnp.max(masked_lse, axis=0), suffix_lse)
    factors = jnp.where(selector[:, :, None], jnp.exp(masked_lse - joint_max[None]), 0.0)
    own_factor = jnp.exp(suffix_lse - joint_max)
    totals = jnp.sum(factors, axis=0) + own_factor
    blended = jnp.einsum("rsh,rhd->shd", factors, flat_out, precision=lax.Precision.HIGHEST)
    blended = blended + own_factor[:, :, None] * suffix_out
    joint_max, totals, blended = joined((joint_max, totals, blended), "sub", combine_halves)
    return (blended / totals[:, :, None]).reshape(seq_local, row_width).astype(jnp.float32)


SENT = jnp.int16
STEPS = 32000.0
TINY = 1e-30
LOG2E = 1.4426950408889634
FIRST_SLOT = (0, 0, 1, 1)
HOLDERS = (((0, 0), (1, 0)), ((1, 1), (2, 0), (3, 0)))
CHUNK = 4
SENDS = ((2, 0), (3, 0), (0, 0), (1, 0), (2, 1), (3, 1), (4, 0), (5, 0), (6, 0), (7, 0))


def windows(chip):
    return (0, 1) if chip == 1 else (FIRST_SLOT[chip],)


def lanes(column, width=HEAD_SIZE):
    return jnp.broadcast_to(column, (column.shape[0], width))


def standing(row):
    return jnp.broadcast_to(row, (HEAD_SIZE, HEAD_SIZE)).T


def attend(
    of_ref, len_ref, suf_ref, table_ref, q_in, pk_ref, pv_ref, sk_ref, sv_ref,
    out_ref,
    prompt_of, prompt_len, suffix_len, page_table, q_ref, order, places, qf, q_send, q_all, kbuf, vbuf, pool_k, pool_v,
    o_send, l_send, o_recv, l_recv, l_cols, suf_w, suf_s, suf_o, suf_l, merged,
    in_sem, own_sem, swap_send, swap_recv, pool_sem, qs_sem, qr_sem, os_sem, or_sem, ls_sem, lr_sem,
    relay_sem, ready_sem, held, held_top,
):
    me = lax.axis_index("kv")
    chip = me // 2
    core = me % 2
    other = 1 - core
    partner = chip * 2 + other
    devices = 8
    rows = q_ref.shape[0]
    most = rows // 2
    heads = pk_ref.shape[1] // HEAD_SIZE
    half = heads // 2
    group = q_ref.shape[1] // (heads * HEAD_SIZE)
    positions = pk_ref.shape[0]
    lines = group * most
    slots = page_table.shape[0]
    span = slots * sk_ref.shape[1]
    scale = LOG2E / math.sqrt(HEAD_SIZE)

    def columns(head):
        return pl.ds(pl.multiple_of(head * HEAD_SIZE, HEAD_SIZE), HEAD_SIZE)

    def signal(semaphore, dst):
        pl.semaphore_signal(semaphore, inc=1, device_id={"kv": dst},
                            device_id_type=pl.DeviceIdType.MESH)

    barrier = pltpu.get_barrier_semaphore()
    for dst in range(devices):
        @pl.when((dst == partner) | (dst // 2 > chip))
        def _():
            signal(barrier, dst)

    pool_copies = [pltpu.make_async_copy(sk_ref, pool_k, pool_sem.at[0]),
                   pltpu.make_async_copy(sv_ref, pool_v, pool_sem.at[1])]
    own_copies = []
    for h in range(half):
        for i, (ref, buf) in enumerate(((pk_ref, kbuf), (pv_ref, vbuf))):
            own_copies.append(pltpu.make_async_copy(
                ref.at[:, columns(core * half + h)], buf.at[core, h], own_sem.at[i]))
    inputs = [pltpu.make_async_copy(src, dst, in_sem.at[i]) for i, (src, dst) in enumerate((
        (of_ref, prompt_of), (len_ref, prompt_len), (suf_ref, suffix_len),
        (table_ref, page_table), (q_in, q_ref)))]
    for copy in inputs:
        copy.start()
    pool_copies[0].start()
    for copy in own_copies:
        copy.start()
    pl.semaphore_wait(barrier, 2 * chip + 1)
    for dst in range(devices):
        @pl.when(dst // 2 < chip)
        def _():
            signal(ready_sem.at[chip], dst)

    def swap_copies():
        made = []
        for h in range(half):
            for i, (ref, buf) in enumerate(((pk_ref, kbuf), (pv_ref, vbuf))):
                made.append(pltpu.make_async_remote_copy(
                    src_ref=ref.at[:, columns(other * half + h)], dst_ref=buf.at[core, h],
                    send_sem=swap_send.at[i], recv_sem=swap_recv.at[i],
                    device_id={"kv": partner}, device_id_type=pl.DeviceIdType.MESH))
        return made

    swaps = swap_copies()
    for copy in swaps:
        copy.start()

    for copy in inputs:
        copy.wait()

    count = [jnp.int32(0), jnp.int32(0)]
    place = []
    for s in range(rows):
        is_one = prompt_of[me * rows + s]
        place.append(jnp.where(is_one == 1, most + count[1], count[0]))
        count[0] = count[0] + (1 - is_one)
        count[1] = count[1] + is_one
        places[s] = place[s]
    row_ids = lax.broadcasted_iota(jnp.int32, (rows, rows), 0)
    col_ids = lax.broadcasted_iota(jnp.int32, (rows, rows), 1)
    chooser = jnp.zeros((rows, rows), jnp.float32)
    for s in range(rows):
        chooser = jnp.where((row_ids == place[s]) & (col_ids == s), 1.0, chooser)
    for r in range(rows):
        found = jnp.int32(0)
        for s in range(rows):
            found = jnp.where(place[s] == r, s, found)
        order[r] = found
    chooser = chooser.astype(jnp.bfloat16)

    for h in range(heads):
        width = group * HEAD_SIZE
        block = jnp.dot(chooser, q_ref[:, h * width:(h + 1) * width],
                        preferred_element_type=jnp.float32)
        for p in range(2):
            tall = jnp.concatenate(
                [block[p * most:(p + 1) * most, g * HEAD_SIZE:(g + 1) * HEAD_SIZE]
                 for g in range(group)], axis=0)
            qf[p, h] = tall
            q_send[p, h] = tall.astype(jnp.bfloat16)

    def query_copy(dst, slot, src):
        prompt = windows(dst // 2)[slot]
        return pltpu.make_async_remote_copy(
            src_ref=q_send.at[prompt, pl.ds(dst % 2 * half, half)], dst_ref=q_all.at[slot, src],
            send_sem=qs_sem.at[slot], recv_sem=qr_sem.at[slot, src // CHUNK],
            device_id={"kv": dst}, device_id_type=pl.DeviceIdType.MESH)

    def send_up(to):
        pl.semaphore_wait(ready_sem.at[to], 2)
        for dst, slot in SENDS:
            if dst // 2 == to:
                query_copy(dst, slot, me).start()

    for dst, slot in SENDS:
        @pl.when((me != dst) & (dst // 2 <= chip) & ((chip < 2) | ((slot == 0) & (dst > 1))))
        def _():
            query_copy(dst, slot, me).start()

        @pl.when(me == dst)
        def _():
            q_all[slot, me] = q_send[windows(dst // 2)[slot], (dst % 2) * half:(dst % 2 + 1) * half]

    @pl.when(chip == 0)
    def _():
        send_up(1)

    @pl.when(chip == 1)
    def _():
        send_up(2)

    @pl.when((chip == 1) | (chip == 2))
    def _():
        send_up(3)

    spots = lax.broadcasted_iota(jnp.int32, (span, HEAD_SIZE), 0)
    lane = lax.broadcasted_iota(jnp.int32, (1, HEAD_SIZE), 1)
    pairs = heads // 2

    def gathered(pool, s, columns_of):
        return jnp.concatenate(
            [pool[page_table[j, s], :, columns_of] for j in range(slots)], axis=0)

    pool_copies[0].wait()
    pool_copies[1].start()

    @pl.when(chip >= 2)
    def _():
        for dst, slot in SENDS:
            if slot == 1:
                query_copy(dst, slot, me).start()

    def suffix_scores(batch):
        p, pair = batch // pairs, batch % pairs
        wanted = pl.ds(pl.multiple_of(pair * 2 * HEAD_SIZE, 2 * HEAD_SIZE), 2 * HEAD_SIZE)
        tall = qf[p, pl.ds(pair * 2, 2)].reshape(2 * lines, HEAD_SIZE).T.astype(jnp.bfloat16)
        scores = None
        length = jnp.zeros((1, HEAD_SIZE), jnp.int32)
        for rank in range(most):
            s = order[p * most + rank]
            mine = lane % most == rank
            length = jnp.where(mine, suffix_len[s], length)
            both = [jnp.where(mine & (lane // lines == i), 1.0, 0.0).astype(jnp.bfloat16)
                    for i in range(2)]
            query = jnp.concatenate([tall * both[0], tall * both[1]], axis=0)
            part = jnp.dot(gathered(pool_k, s, wanted), query, preferred_element_type=jnp.float32)
            scores = part if scores is None else scores + part
        scores = jnp.where(spots < length, scores * scale, NEGATIVE)
        top = jnp.max(scores, axis=0, keepdims=True)
        weights = jnp.exp2(scores - top)
        total = jnp.sum(weights, axis=0, keepdims=True)
        suf_w[batch] = weights.T.astype(jnp.bfloat16)
        suf_s[batch, 0:1] = top + jnp.log2(total)
        suf_s[batch, 1:2] = 1.0 / total

    def suffix_half(p):
        for pair in range(pairs):
            suffix_scores(p * pairs + pair)

    @pl.loop(0, jnp.where(chip == 1, 1, 2))
    def _(p):
        suffix_half(p)

        @pl.when((chip == 0) & (p == 0))
        def _():
            for to in (2, 3):
                send_up(to)

    def both_heads(i):
        buf = (kbuf, vbuf)[i]
        return pltpu.make_async_remote_copy(
            src_ref=buf.at[core], dst_ref=buf.at[core], send_sem=swap_send.at[i],
            recv_sem=swap_recv.at[i], device_id={"kv": partner},
            device_id_type=pl.DeviceIdType.MESH)

    for i, buf in enumerate((kbuf, vbuf)):
        pltpu.make_async_copy(buf.at[core], buf.at[core], own_sem.at[i]).wait()
        both_heads(i).wait_recv()

    first_end = prompt_len[0]
    second_end = first_end + prompt_len[1]

    def query_span(slot, turn, number):
        return pltpu.make_async_remote_copy(
            src_ref=q_all.at[slot, pl.ds(0, number)], dst_ref=q_all.at[slot, pl.ds(0, number)],
            send_sem=qs_sem.at[slot], recv_sem=qr_sem.at[slot, turn],
            device_id={"kv": partner}, device_id_type=pl.DeviceIdType.MESH)

    def relay_copy(offset):
        src = CHUNK + offset
        return pltpu.make_async_remote_copy(
            src_ref=q_all.at[0, src], dst_ref=q_all.at[0, src],
            send_sem=relay_sem.at[0], recv_sem=qr_sem.at[0, 1],
            device_id={"kv": core}, device_id_type=pl.DeviceIdType.MESH)

    def head_copy(dst, slot, h):
        group = 2 if slot == 1 else me // CHUNK
        return pltpu.make_async_remote_copy(
            src_ref=o_send.at[slot, dst, h], dst_ref=o_recv.at[slot, me, h],
            send_sem=os_sem.at[slot], recv_sem=or_sem.at[group, core],
            device_id={"kv": dst}, device_id_type=pl.DeviceIdType.MESH)

    def facts_copy(dst, slot):
        group = 2 if slot == 1 else me // CHUNK
        return pltpu.make_async_remote_copy(
            src_ref=l_send.at[slot, dst], dst_ref=l_recv.at[slot, me],
            send_sem=ls_sem.at[slot], recv_sem=lr_sem.at[group, core],
            device_id={"kv": dst}, device_id_type=pl.DeviceIdType.MESH)

    def back_spans(slot, group, d, number):
        return [pltpu.make_async_remote_copy(
            src_ref=sent.at[slot, pl.ds(0, number)], dst_ref=got.at[slot, pl.ds(0, number)],
            send_sem=left.at[slot], recv_sem=landed.at[group, d],
            device_id={"kv": partner}, device_id_type=pl.DeviceIdType.MESH)
            for sent, got, left, landed in ((o_send, o_recv, os_sem, or_sem), (l_send, l_recv, ls_sem, lr_sem))]

    def wait_back(slot, group, d, number):
        for span_copy in back_spans(slot, group, d, number):
            span_copy.wait_recv()

    is_level = lax.broadcasted_iota(jnp.int32, (CHUNK * lines, HEAD_SIZE), 1) % 2 == 0

    def prompt_turn(slot, turn, low, high, first_block):
        blocks = 2 - first_block
        spot = (chip * 2 + first_block) * positions + lax.broadcasted_iota(
            jnp.int32, (1, blocks * positions), 1)
        bias = jnp.where((spot >= low) & (spot < high), 0.0, NEGATIVE)
        begin = turn * CHUNK

        waits = (chip != 1) | (turn == 0) | (slot == 1)

        @pl.when(me // CHUNK == turn)
        def _():
            query_span(slot, turn, CHUNK - 1).wait_recv()

        @pl.when((me // CHUNK != turn) & waits)
        def _():
            query_span(slot, turn, CHUNK).wait_recv()

        width = blocks * positions

        def scored(h):
            query = q_all[slot, pl.ds(begin, CHUNK), h].reshape(CHUNK * lines, HEAD_SIZE)
            keys = kbuf[first_block:2, h].reshape(width, HEAD_SIZE)
            scores = lax.dot_general(query, keys, (((1,), (1,)), ((), ())),
                                     preferred_element_type=jnp.float32)
            scores = scores * scale + bias
            return scores, lanes(jnp.max(scores, axis=1, keepdims=True))

        def finished(h, scores, top):
            values = vbuf[first_block:2, h].reshape(width, HEAD_SIZE)
            weights = jnp.exp2(scores - jnp.concatenate([top] * (width // HEAD_SIZE), axis=1))
            total = jnp.sum(weights, axis=1, keepdims=True)
            mixed = jnp.dot(weights.astype(jnp.bfloat16), values,
                            preferred_element_type=jnp.float32)
            peak = jnp.maximum(jnp.max(jnp.abs(mixed), axis=1, keepdims=True), TINY)
            steps = jnp.round(mixed * (STEPS / peak)).astype(jnp.int32)
            o_send[slot, pl.ds(begin, CHUNK), h] = steps.astype(SENT).reshape(
                CHUNK, lines, HEAD_SIZE)
            peak = peak * (1.0 / (STEPS * total))
            facts = jnp.where(is_level, top + lanes(jnp.log2(total)), lanes(peak))
            l_cols[pl.ds(begin, CHUNK), h] = facts.reshape(CHUNK, lines, HEAD_SIZE)

        def returned(h):
            @pl.loop(0, CHUNK)
            def _(offset):
                @pl.when(me != begin + offset)
                def _():
                    head_copy(begin + offset, slot, h).start()

        ready = scored(0)
        for h in range(half):
            finished(h, *ready)
            if h + 1 < half:
                scores, top = scored(h + 1)
                held[:, :width] = scores
                held_top[...] = top
            if slot == 1 and h == 0:
                @pl.when(turn == 0)
                def _():
                    query_span(0, 1, CHUNK).wait_recv()
                    for i in range(CHUNK):
                        relay_copy(i).start()
            returned(h)
            if h + 1 < half:
                ready = (held[:, :width], held_top[...])

        @pl.loop(0, CHUNK)
        def _(offset):
            dst = begin + offset
            turned = l_cols[dst].reshape(half * lines, HEAD_SIZE).T
            l_send[slot, dst] = turned[0:2]

            @pl.when(me != dst)
            def _():
                facts_copy(dst, slot).start()

            @pl.when(me == dst)
            def _():
                o_recv[slot, me] = o_send[slot, dst]
                l_recv[slot, me] = l_send[slot, dst]

    low, high = jnp.where(chip < 2, 0, first_end), jnp.where(chip < 2, first_end, second_end)
    row = lax.broadcasted_iota(jnp.int32, (2 * lines, HEAD_SIZE), 0)

    def suffix_values():
        pool_copies[1].wait()

        @pl.loop(0, 2 * pairs)
        def _(batch):
            p, pair = batch // pairs, batch % pairs
            wanted = pl.ds(pl.multiple_of(pair * 2 * HEAD_SIZE, 2 * HEAD_SIZE), 2 * HEAD_SIZE)
            weights = suf_w[batch]
            mixed = None
            for rank in range(most):
                s = order[p * most + rank]
                mine = jnp.where(row % most == rank, 1.0, 0.0).astype(jnp.bfloat16)
                mine = jnp.concatenate([mine] * (span // HEAD_SIZE), axis=1)
                part = jnp.dot(weights * mine, gathered(pool_v, s, wanted),
                               preferred_element_type=jnp.float32)
                mixed = part if mixed is None else mixed + part
            level, inverse = standing(suf_s[batch, 0:1]), standing(suf_s[batch, 1:2])
            for i in range(2):
                mine = slice(i * lines, (i + 1) * lines)
                suf_o[p, pair * 2 + i] = (
                    mixed[mine, i * HEAD_SIZE:(i + 1) * HEAD_SIZE] * inverse[mine])
                suf_l[p, pair * 2 + i] = level[mine]

    @pl.loop(0, 2)
    def _(step):
        @pl.when(chip == 1)
        def _():
            prompt_turn(1, step, first_end, second_end, 1)

        prompt_turn(0, jnp.where(chip == 1, 1 - step, step), low, high, 0)

        @pl.when((chip == 1) & (step == 1))
        def _():
            suffix_half(1)

        @pl.when(step == jnp.where(chip == 1, 1, 0))
        def _():
            suffix_values()

    for p in range(2):
        for d in range(2):
            arrived, levels = [], []
            if p == 1:
                @pl.when(me != 2 + d)
                def _():
                    wait_back(1, 2, d, 1)

            inside = (me // CHUNK == p) & (core == d)

            @pl.when(inside)
            def _():
                wait_back(0, p, d, 1)

            @pl.when(jnp.logical_not(inside))
            def _():
                wait_back(0, p, d, 2)

            for c, slot in HOLDERS[p]:
                sender = 2 * c + d
                levels.append((standing(l_recv[slot, sender, 0:1]), standing(l_recv[slot, sender, 1:2])))
                arrived.append((slot, sender))
            for hh in range(half):
                h = d * half + hh
                mine = slice(hh * lines, (hh + 1) * lines)
                parts = [(level[mine], o_recv[slot, sender, hh].astype(jnp.int32).astype(jnp.float32)
                          * step[mine])
                         for (level, step), (slot, sender) in zip(levels, arrived)]
                parts.append((suf_l[p, h], suf_o[p, h]))
                joint = functools.reduce(jnp.maximum, [level for level, _ in parts])
                factors = [jnp.exp2(level - joint) for level, _ in parts]
                total = functools.reduce(jnp.add, factors)
                blend = functools.reduce(jnp.add, [f * o for f, (_, o) in zip(factors, parts)])
                blend = blend / total
                for g in range(group):
                    first = (h * group + g) * HEAD_SIZE
                    merged[p * most:(p + 1) * most, first:first + HEAD_SIZE] = (
                        blend[g * most:(g + 1) * most])

    for s in range(rows):
        out_ref[s:s + 1, :] = merged[pl.ds(places[s], 1), :]

    for i in range(2):
        both_heads(i).wait_send()

    @pl.when(chip < 2)
    def _():
        query_span(0, 0, devices - 1).wait_send()

    @pl.when(chip >= 2)
    def _():
        query_span(0, 0, devices - 3).wait_send()

    @pl.when(chip == 1)
    def _():
        query_span(1, 0, 1).wait_send()
        pltpu.make_async_remote_copy(
            src_ref=q_all.at[0, pl.ds(CHUNK, CHUNK)], dst_ref=q_all.at[0, pl.ds(CHUNK, CHUNK)],
            send_sem=relay_sem.at[0], recv_sem=qr_sem.at[0, 1],
            device_id={"kv": core}, device_id_type=pl.DeviceIdType.MESH).wait_send()
        for span_copy in back_spans(1, 2, 0, devices - 1):
            span_copy.wait_send()

    @pl.when(chip != 1)
    def _():
        query_span(1, 0, 2).wait_send()

    for span_copy in back_spans(0, 0, 0, devices - 1):
        span_copy.wait_send()


def fused(
    queries,
    prompt_of,
    prompt_len,
    suffix_len,
    page_table,
    prompt_keys,
    shared_prompt_values,
    suffix_pool_keys,
    suffix_pool_values,
):
    rows, width = queries.shape
    most = rows // 2
    positions, depth = prompt_keys.shape
    heads = depth // HEAD_SIZE
    half = heads // 2
    group = width // depth
    lines = group * most
    span = page_table.shape[1] * suffix_pool_keys.shape[1]
    devices = lax.axis_size("kv")
    f32, bf16 = jnp.float32, jnp.bfloat16
    vmem, dma = pltpu.VMEM, pltpu.SemaphoreType.DMA
    return pl.pallas_call(
        attend,
        out_shape=pltpu.VMEM((rows, width), f32),
        in_specs=[pl.BlockSpec(memory_space=pl.ANY)] * 9,
        out_specs=pl.BlockSpec(memory_space=pltpu.VMEM),
        scratch_shapes=[
            pltpu.SMEM(prompt_of.shape[:1], jnp.int32),
            pltpu.SMEM(prompt_len.shape, jnp.int32),
            pltpu.SMEM(suffix_len.shape, jnp.int32),
            pltpu.SMEM(page_table.shape[::-1], jnp.int32),
            vmem((rows, width), bf16),
            pltpu.SMEM((rows,), jnp.int32),
            pltpu.SMEM((rows,), jnp.int32),
            vmem((2, heads, lines, HEAD_SIZE), f32),
            vmem((2, heads, lines, HEAD_SIZE), bf16),
            vmem((2, devices, half, lines, HEAD_SIZE), bf16),
            vmem((2, half, positions, HEAD_SIZE), bf16),
            vmem((2, half, positions, HEAD_SIZE), bf16),
            vmem(suffix_pool_keys.shape, bf16),
            vmem(suffix_pool_values.shape, bf16),
            vmem((2, devices, half, lines, HEAD_SIZE), SENT),
            vmem((2, devices, 2, HEAD_SIZE), f32),
            vmem((2, devices, half, lines, HEAD_SIZE), SENT),
            vmem((2, devices, 2, HEAD_SIZE), f32),
            vmem((devices, half, lines, HEAD_SIZE), f32),
            vmem((heads, 2 * lines, span), bf16),
            vmem((heads, 2, HEAD_SIZE), f32),
            vmem((2, heads, lines, HEAD_SIZE), f32),
            vmem((2, heads, lines, HEAD_SIZE), f32),
            vmem((rows, width), f32),
            dma((5,)),
            dma((2,)),
            dma((2,)),
            dma((2,)),
            dma((2,)),
            dma((2,)),
            dma((2, 2)),
            dma((2,)),
            dma((3, 2)),
            dma((2,)),
            dma((3, 2)),
            dma((1,)),
            pltpu.SemaphoreType.REGULAR((devices // 2,)),
            vmem((CHUNK * lines, 2 * positions), f32),
            vmem((CHUNK * lines, HEAD_SIZE), f32),
        ],
        compiler_params=pltpu.CompilerParams(
            collective_id=0, has_side_effects=True, vmem_limit_bytes=48 * 1024 * 1024
        ),
    )(
        *(pltpu.with_memory_space_constraint(array, pltpu.HBM) for array in (
            prompt_of.reshape(-1), prompt_len, suffix_len, page_table.T,
            queries, prompt_keys, shared_prompt_values, suffix_pool_keys, suffix_pool_values))
    )


def fits(mesh):
    return mesh.shape["kv"] == 8 and mesh.shape["sub"] == 1


def solution(mesh):
    body = fused if fits(mesh) else shards
    placed = (
        P(("grp", "kv"), "hd"),
        P("grp", None),
        P("grp"),
        P(("grp", "kv")),
        P(("grp", "kv"), "sub"),
        P(("grp", "kv", "sub"), "hd"),
        P(("grp", "kv", "sub"), "hd"),
        P(("grp", "kv", "sub"), None, "hd"),
        P(("grp", "kv", "sub"), None, "hd"),
    )
    return jax.shard_map(
        body, mesh=mesh, in_specs=placed, out_specs=P(("grp", "kv"), "hd"), check_vma=False
    )
```

```python
import functools
import math

import jax
import jax.numpy as jnp
from jax import lax
from jax.experimental import pallas as pl
from jax.experimental.pallas import tpu as pltpu
from jax.sharding import PartitionSpec as P

HEAD_SIZE = 128


NEGATIVE = -1e30


def joined(value, axis, combine):
    everything = jax.tree.map(lambda part: lax.all_gather(part, axis), value)
    leading = jax.tree.map(lambda part: part[0], everything)

    def hop(k, so_far):
        return combine(so_far, jax.tree.map(lambda part: part[k], everything))

    return lax.fori_loop(1, lax.axis_size(axis), hop, leading)


def attend_block(sent_rows, key_block, value_block, lower_bound, upper_bound, first_position):
    row_count = sent_rows.shape[0]
    key_count = key_block.shape[0]
    kv_local = key_block.shape[1] // HEAD_SIZE
    query_group_size = sent_rows.shape[1] // (HEAD_SIZE * kv_local)
    position = first_position + jnp.arange(key_count, dtype=jnp.int32)
    key_mask = (position[None, :] >= lower_bound[:, None]) & (
        position[None, :] < upper_bound[:, None]
    )
    key_mask = key_mask[:, None, :]
    score_scale = 1.0 / math.sqrt(HEAD_SIZE)
    blended_parts = []
    lse_parts = []
    for kv_head in range(kv_local):
        low_column = kv_head * query_group_size * HEAD_SIZE
        head_query = sent_rows[:, low_column : low_column + query_group_size * HEAD_SIZE].reshape(
            row_count * query_group_size, HEAD_SIZE
        )
        head_keys = key_block[:, kv_head * HEAD_SIZE : (kv_head + 1) * HEAD_SIZE]
        head_values = value_block[:, kv_head * HEAD_SIZE : (kv_head + 1) * HEAD_SIZE]
        scores = lax.dot_general(
            head_query, head_keys, (((1,), (1,)), ((), ())), preferred_element_type=jnp.float32
        )
        scores = (scores * score_scale).reshape(row_count, query_group_size, key_count)
        scores = jnp.where(key_mask, scores, NEGATIVE)
        row_max = jnp.max(scores, axis=2, keepdims=True)
        weights = jnp.where(key_mask, jnp.exp(scores - row_max), 0.0)
        totals = jnp.maximum(jnp.sum(weights, axis=2), 1.0)
        weighted = jnp.dot(
            weights.astype(jnp.bfloat16).reshape(row_count * query_group_size, key_count),
            head_values,
            preferred_element_type=jnp.float32,
        )
        weighted = weighted.reshape(row_count, query_group_size, HEAD_SIZE) / totals[:, :, None]
        blended_parts.append(weighted.reshape(row_count, query_group_size * HEAD_SIZE))
        lse_parts.append(row_max[:, :, 0] + jnp.log(totals))
    return (jnp.concatenate(blended_parts, axis=1), jnp.concatenate(lse_parts, axis=1))


def combine_halves(earlier, later):
    joint_max = jnp.maximum(earlier[0], later[0])
    left_factor = jnp.exp(earlier[0] - joint_max)
    right_factor = jnp.exp(later[0] - joint_max)
    totals = earlier[1] * left_factor + later[1] * right_factor
    blended = earlier[2] * left_factor[:, :, None] + later[2] * right_factor[:, :, None]
    return (joint_max, totals, blended)


def shards(
    queries,
    prompt_of,
    prompt_len,
    suffix_len,
    page_table,
    prompt_keys,
    shared_prompt_values,
    suffix_pool_keys,
    suffix_pool_values,
):
    kv_count = lax.axis_size("kv")
    sub_count = lax.axis_size("sub")
    kv_index = lax.axis_index("kv")
    sub_index = lax.axis_index("sub")
    seq_local = queries.shape[0]
    row_width = queries.shape[1]
    heads_local = row_width // HEAD_SIZE
    cache_local = prompt_keys.shape[0]
    kv_reach = sub_count * cache_local
    prompt_count = prompt_len.shape[0]
    prompt_starts = jnp.cumsum(prompt_len) - prompt_len
    prompt_ends = prompt_starts + prompt_len
    prompt_labels = jnp.arange(prompt_count, dtype=jnp.int32)
    range_low = jnp.arange(kv_count, dtype=jnp.int32) * kv_reach
    intersections = (prompt_starts[None, :] < range_low[:, None] + kv_reach) & (
        prompt_ends[None, :] > range_low[:, None]
    )
    later_slot = prompt_starts[None, :] > range_low[:, None]
    first_position = (kv_index * sub_count + sub_index) * cache_local
    most_rows = seq_local // prompt_count
    owned_prompt = lax.dynamic_slice_in_dim(prompt_of[:, 0], kv_index * seq_local, seq_local)
    prompt_hits = owned_prompt[:, None] == prompt_labels[None, :]
    hit_counts = prompt_hits.astype(jnp.int32)
    ranks = jnp.sum((jnp.cumsum(hit_counts, axis=0) - hit_counts) * hit_counts, axis=1)
    seq_intersection = jnp.any(intersections[:, None, :] & prompt_hits[None, :, :], axis=2)
    seq_later = jnp.any(later_slot[:, None, :] & prompt_hits[None, :, :], axis=2).astype(jnp.int32)
    slot_labels = jnp.arange(2, dtype=jnp.int32)
    rank_labels = jnp.arange(most_rows, dtype=jnp.int32)
    selector = seq_intersection[:, None, None, :] & (
        seq_later[:, None, None, :] == slot_labels[None, :, None, None]
    )
    selector = selector & (ranks[None, None, None, :] == rank_labels[None, None, :, None])
    selector = selector.reshape(kv_count * 2 * most_rows, seq_local)
    outgoing = jnp.dot(
        selector.astype(jnp.bfloat16), queries, preferred_element_type=jnp.float32
    ).astype(jnp.bfloat16)
    incoming = lax.all_to_all(
        outgoing.reshape(kv_count, 2 * most_rows, row_width),
        "kv",
        split_axis=0,
        concat_axis=0,
        tiled=True,
    )
    mine_intersection = lax.dynamic_index_in_dim(intersections, kv_index, 0, keepdims=False)
    mine_later = lax.dynamic_index_in_dim(later_slot, kv_index, 0, keepdims=False).astype(jnp.int32)
    chosen = mine_intersection[None, :] & (mine_later[None, :] == slot_labels[:, None])
    slot_low = jnp.sum(jnp.where(chosen, prompt_starts[None, :], 0), axis=1)
    slot_high = jnp.sum(jnp.where(chosen, prompt_ends[None, :], 0), axis=1)
    lower_bound = jnp.broadcast_to(
        jnp.repeat(slot_low, most_rows)[None, :], (kv_count, 2 * most_rows)
    ).reshape(-1)
    upper_bound = jnp.broadcast_to(
        jnp.repeat(slot_high, most_rows)[None, :], (kv_count, 2 * most_rows)
    ).reshape(-1)
    sent_rows = incoming.reshape(kv_count * 2 * most_rows, row_width)
    back_rows = 2 * most_rows
    prompt_out, prompt_lse = attend_block(
        sent_rows, prompt_keys, shared_prompt_values, lower_bound, upper_bound, first_position
    )
    returned_out, returned_lse = (
        lax.all_to_all(
            prompt_out.reshape(kv_count, back_rows, row_width),
            "kv",
            split_axis=0,
            concat_axis=0,
            tiled=True,
        ),
        lax.all_to_all(
            prompt_lse.reshape(kv_count, back_rows, heads_local),
            "kv",
            split_axis=0,
            concat_axis=0,
            tiled=True,
        ),
    )
    page_slots = page_table.shape[1]
    page_length = suffix_pool_keys.shape[1]
    suffix_span = page_slots * page_length
    gathered_keys = suffix_pool_keys[page_table].reshape(seq_local, suffix_span, -1)
    gathered_values = suffix_pool_values[page_table].reshape(seq_local, suffix_span, -1)
    suffix_first = sub_index * suffix_span

    def one_sequence(query_line, seq_keys, seq_values, seq_length):
        return attend_block(
            query_line[None, :],
            seq_keys,
            seq_values,
            jnp.zeros((1,), jnp.int32),
            seq_length[None],
            suffix_first,
        )

    suffix_out, suffix_lse = jax.vmap(one_sequence)(
        queries, gathered_keys, gathered_values, suffix_len
    )
    suffix_out = suffix_out[:, 0].reshape(seq_local, heads_local, HEAD_SIZE)
    suffix_lse = suffix_lse[:, 0]
    flat_lse = returned_lse.reshape(-1, heads_local)
    flat_out = returned_out.reshape(-1, heads_local, HEAD_SIZE)
    masked_lse = jnp.where(selector[:, :, None], flat_lse[:, None, :], NEGATIVE)
    joint_max = jnp.maximum(jnp.max(masked_lse, axis=0), suffix_lse)
    factors = jnp.where(selector[:, :, None], jnp.exp(masked_lse - joint_max[None]), 0.0)
    own_factor = jnp.exp(suffix_lse - joint_max)
    totals = jnp.sum(factors, axis=0) + own_factor
    blended = jnp.einsum("rsh,rhd->shd", factors, flat_out, precision=lax.Precision.HIGHEST)
    blended = blended + own_factor[:, :, None] * suffix_out
    joint_max, totals, blended = joined((joint_max, totals, blended), "sub", combine_halves)
    return (blended / totals[:, :, None]).reshape(seq_local, row_width).astype(jnp.float32)


SENT = jnp.int16
STEPS = 32000.0
TINY = 1e-30
LOG2E = 1.4426950408889634
FIRST_SLOT = (0, 0, 1, 1)
HOLDERS = (((0, 0), (1, 0)), ((1, 1), (2, 0), (3, 0)))
CHUNK = 4
SENDS = ((2, 0), (3, 0), (0, 0), (1, 0), (2, 1), (3, 1), (4, 0), (5, 0), (6, 0), (7, 0))


def windows(chip):
    return (0, 1) if chip == 1 else (FIRST_SLOT[chip],)


def lanes(column, width=HEAD_SIZE):
    return jnp.broadcast_to(column, (column.shape[0], width))


def standing(row):
    return jnp.broadcast_to(row, (HEAD_SIZE, HEAD_SIZE)).T


def attend(
    of_ref, len_ref, suf_ref, table_ref, q_in, pk_ref, pv_ref, sk_ref, sv_ref,
    out_ref,
    prompt_of, prompt_len, suffix_len, page_table, q_ref, order, places, qf, q_send, q_all, kbuf, vbuf, pool_k, pool_v,
    o_send, l_send, o_recv, l_recv, l_cols, suf_w, suf_s, suf_o, suf_l, merged,
    in_sem, own_sem, swap_send, swap_recv, pool_sem, qs_sem, qr_sem, os_sem, or_sem, ls_sem, lr_sem,
    relay_sem, ready_sem, held, held_top,
):
    me = lax.axis_index("kv")
    chip = me // 2
    core = me % 2
    other = 1 - core
    partner = chip * 2 + other
    devices = 8
    rows = q_ref.shape[0]
    most = rows // 2
    heads = pk_ref.shape[1] // HEAD_SIZE
    half = heads // 2
    group = q_ref.shape[1] // (heads * HEAD_SIZE)
    positions = pk_ref.shape[0]
    lines = group * most
    slots = page_table.shape[0]
    span = slots * sk_ref.shape[1]
    scale = LOG2E / math.sqrt(HEAD_SIZE)

    def columns(head):
        return pl.ds(pl.multiple_of(head * HEAD_SIZE, HEAD_SIZE), HEAD_SIZE)

    def signal(semaphore, dst):
        pl.semaphore_signal(semaphore, inc=1, device_id={"kv": dst},
                            device_id_type=pl.DeviceIdType.MESH)

    barrier = pltpu.get_barrier_semaphore()
    for dst in range(devices):
        @pl.when((dst == partner) | (dst // 2 > chip))
        def _():
            signal(barrier, dst)

    pool_copies = [pltpu.make_async_copy(sk_ref, pool_k, pool_sem.at[0]),
                   pltpu.make_async_copy(sv_ref, pool_v, pool_sem.at[1])]
    own_copies = []
    for h in range(half):
        for i, (ref, buf) in enumerate(((pk_ref, kbuf), (pv_ref, vbuf))):
            own_copies.append(pltpu.make_async_copy(
                ref.at[:, columns(core * half + h)], buf.at[core, h], own_sem.at[i]))
    inputs = [pltpu.make_async_copy(src, dst, in_sem.at[i]) for i, (src, dst) in enumerate((
        (of_ref, prompt_of), (len_ref, prompt_len), (suf_ref, suffix_len),
        (table_ref, page_table), (q_in, q_ref)))]
    for copy in inputs:
        copy.start()
    pool_copies[0].start()
    for copy in own_copies:
        copy.start()
    pl.semaphore_wait(barrier, 2 * chip + 1)
    for dst in range(devices):
        @pl.when(dst // 2 < chip)
        def _():
            signal(ready_sem.at[chip], dst)

    def swap_copies():
        made = []
        for h in range(half):
            for i, (ref, buf) in enumerate(((pk_ref, kbuf), (pv_ref, vbuf))):
                made.append(pltpu.make_async_remote_copy(
                    src_ref=ref.at[:, columns(other * half + h)], dst_ref=buf.at[core, h],
                    send_sem=swap_send.at[i], recv_sem=swap_recv.at[i],
                    device_id={"kv": partner}, device_id_type=pl.DeviceIdType.MESH))
        return made

    swaps = swap_copies()
    for copy in swaps:
        copy.start()

    for copy in inputs:
        copy.wait()

    count = [jnp.int32(0), jnp.int32(0)]
    place = []
    for s in range(rows):
        is_one = prompt_of[me * rows + s]
        place.append(jnp.where(is_one == 1, most + count[1], count[0]))
        count[0] = count[0] + (1 - is_one)
        count[1] = count[1] + is_one
        places[s] = place[s]
    row_ids = lax.broadcasted_iota(jnp.int32, (rows, rows), 0)
    col_ids = lax.broadcasted_iota(jnp.int32, (rows, rows), 1)
    chooser = jnp.zeros((rows, rows), jnp.float32)
    for s in range(rows):
        chooser = jnp.where((row_ids == place[s]) & (col_ids == s), 1.0, chooser)
    for r in range(rows):
        found = jnp.int32(0)
        for s in range(rows):
            found = jnp.where(place[s] == r, s, found)
        order[r] = found
    chooser = chooser.astype(jnp.bfloat16)

    for h in range(heads):
        width = group * HEAD_SIZE
        block = jnp.dot(chooser, q_ref[:, h * width:(h + 1) * width],
                        preferred_element_type=jnp.float32)
        for p in range(2):
            tall = jnp.concatenate(
                [block[p * most:(p + 1) * most, g * HEAD_SIZE:(g + 1) * HEAD_SIZE]
                 for g in range(group)], axis=0)
            qf[p, h] = tall
            q_send[p, h] = tall.astype(jnp.bfloat16)

    def query_copy(dst, slot, src):
        prompt = windows(dst // 2)[slot]
        return pltpu.make_async_remote_copy(
            src_ref=q_send.at[prompt, pl.ds(dst % 2 * half, half)], dst_ref=q_all.at[slot, src],
            send_sem=qs_sem.at[slot], recv_sem=qr_sem.at[slot, src // CHUNK],
            device_id={"kv": dst}, device_id_type=pl.DeviceIdType.MESH)

    def send_up(to):
        pl.semaphore_wait(ready_sem.at[to], 2)
        for dst, slot in SENDS[::-1]:
            if dst // 2 == to:
                query_copy(dst, slot, me).start()

    for dst, slot in SENDS:
        @pl.when((me != dst) & (dst // 2 <= chip) & ((chip < 2) | ((slot == 0) & (dst > 1))))
        def _():
            query_copy(dst, slot, me).start()

        @pl.when(me == dst)
        def _():
            q_all[slot, me] = q_send[windows(dst // 2)[slot], (dst % 2) * half:(dst % 2 + 1) * half]

    @pl.when(chip == 0)
    def _():
        send_up(1)

    @pl.when(chip == 1)
    def _():
        send_up(2)

    @pl.when((chip == 1) | (chip == 2))
    def _():
        send_up(3)

    spots = lax.broadcasted_iota(jnp.int32, (span, HEAD_SIZE), 0)
    lane = lax.broadcasted_iota(jnp.int32, (1, HEAD_SIZE), 1)
    pairs = heads // 2

    def gathered(pool, s, columns_of):
        return jnp.concatenate(
            [pool[page_table[j, s], :, columns_of] for j in range(slots)], axis=0)

    pool_copies[0].wait()
    pool_copies[1].start()

    @pl.when(chip >= 2)
    def _():
        for dst, slot in SENDS:
            if slot == 1:
                query_copy(dst, slot, me).start()

    def suffix_scores(batch):
        p, pair = batch // pairs, batch % pairs
        wanted = pl.ds(pl.multiple_of(pair * 2 * HEAD_SIZE, 2 * HEAD_SIZE), 2 * HEAD_SIZE)
        tall = qf[p, pl.ds(pair * 2, 2)].reshape(2 * lines, HEAD_SIZE).T.astype(jnp.bfloat16)
        scores = None
        length = jnp.zeros((1, HEAD_SIZE), jnp.int32)
        for rank in range(most):
            s = order[p * most + rank]
            mine = lane % most == rank
            length = jnp.where(mine, suffix_len[s], length)
            both = [jnp.where(mine & (lane // lines == i), 1.0, 0.0).astype(jnp.bfloat16)
                    for i in range(2)]
            query = jnp.concatenate([tall * both[0], tall * both[1]], axis=0)
            part = jnp.dot(gathered(pool_k, s, wanted), query, preferred_element_type=jnp.float32)
            scores = part if scores is None else scores + part
        scores = jnp.where(spots < length, scores * scale, NEGATIVE)
        top = jnp.max(scores, axis=0, keepdims=True)
        weights = jnp.exp2(scores - top)
        total = jnp.sum(weights, axis=0, keepdims=True)
        suf_w[batch] = weights.T.astype(jnp.bfloat16)
        suf_s[batch, 0:1] = top + jnp.log2(total)
        suf_s[batch, 1:2] = 1.0 / total

    def suffix_half(p):
        for pair in range(pairs):
            suffix_scores(p * pairs + pair)

    @pl.loop(0, jnp.where(chip == 1, 1, 2))
    def _(p):
        suffix_half(p)

        @pl.when((chip == 0) & (p == 0))
        def _():
            for to in (2, 3):
                send_up(to)

    def both_heads(i):
        buf = (kbuf, vbuf)[i]
        return pltpu.make_async_remote_copy(
            src_ref=buf.at[core], dst_ref=buf.at[core], send_sem=swap_send.at[i],
            recv_sem=swap_recv.at[i], device_id={"kv": partner},
            device_id_type=pl.DeviceIdType.MESH)

    for i, buf in enumerate((kbuf, vbuf)):
        pltpu.make_async_copy(buf.at[core], buf.at[core], own_sem.at[i]).wait()
        both_heads(i).wait_recv()

    first_end = prompt_len[0]
    second_end = first_end + prompt_len[1]

    def query_span(slot, turn, number):
        return pltpu.make_async_remote_copy(
            src_ref=q_all.at[slot, pl.ds(0, number)], dst_ref=q_all.at[slot, pl.ds(0, number)],
            send_sem=qs_sem.at[slot], recv_sem=qr_sem.at[slot, turn],
            device_id={"kv": partner}, device_id_type=pl.DeviceIdType.MESH)

    def relay_copy(offset):
        src = CHUNK + offset
        return pltpu.make_async_remote_copy(
            src_ref=q_all.at[0, src], dst_ref=q_all.at[0, src],
            send_sem=relay_sem.at[0], recv_sem=qr_sem.at[0, 1],
            device_id={"kv": core}, device_id_type=pl.DeviceIdType.MESH)

    def head_copy(dst, slot, h):
        group = 2 if slot == 1 else me // CHUNK
        return pltpu.make_async_remote_copy(
            src_ref=o_send.at[slot, dst, h], dst_ref=o_recv.at[slot, me, h],
            send_sem=os_sem.at[slot], recv_sem=or_sem.at[group, core],
            device_id={"kv": dst}, device_id_type=pl.DeviceIdType.MESH)

    def facts_copy(dst, slot):
        group = 2 if slot == 1 else me // CHUNK
        return pltpu.make_async_remote_copy(
            src_ref=l_send.at[slot, dst], dst_ref=l_recv.at[slot, me],
            send_sem=ls_sem.at[slot], recv_sem=lr_sem.at[group, core],
            device_id={"kv": dst}, device_id_type=pl.DeviceIdType.MESH)

    def back_spans(slot, group, d, number):
        return [pltpu.make_async_remote_copy(
            src_ref=sent.at[slot, pl.ds(0, number)], dst_ref=got.at[slot, pl.ds(0, number)],
            send_sem=left.at[slot], recv_sem=landed.at[group, d],
            device_id={"kv": partner}, device_id_type=pl.DeviceIdType.MESH)
            for sent, got, left, landed in ((o_send, o_recv, os_sem, or_sem), (l_send, l_recv, ls_sem, lr_sem))]

    def wait_back(slot, group, d, number):
        for span_copy in back_spans(slot, group, d, number):
            span_copy.wait_recv()

    is_level = lax.broadcasted_iota(jnp.int32, (CHUNK * lines, HEAD_SIZE), 1) % 2 == 0

    def prompt_turn(slot, turn, low, high, first_block):
        blocks = 2 - first_block
        spot = (chip * 2 + first_block) * positions + lax.broadcasted_iota(
            jnp.int32, (1, blocks * positions), 1)
        bias = jnp.where((spot >= low) & (spot < high), 0.0, NEGATIVE)
        begin = turn * CHUNK

        waits = (chip != 1) | (turn == 0) | (slot == 1)

        @pl.when(me // CHUNK == turn)
        def _():
            query_span(slot, turn, CHUNK - 1).wait_recv()

        @pl.when((me // CHUNK != turn) & waits)
        def _():
            query_span(slot, turn, CHUNK).wait_recv()

        width = blocks * positions

        def scored(h):
            query = q_all[slot, pl.ds(begin, CHUNK), h].reshape(CHUNK * lines, HEAD_SIZE)
            keys = kbuf[first_block:2, h].reshape(width, HEAD_SIZE)
            scores = lax.dot_general(query, keys, (((1,), (1,)), ((), ())),
                                     preferred_element_type=jnp.float32)
            scores = scores * scale + bias
            return scores, lanes(jnp.max(scores, axis=1, keepdims=True))

        def finished(h, scores, top):
            values = vbuf[first_block:2, h].reshape(width, HEAD_SIZE)
            weights = jnp.exp2(scores - jnp.concatenate([top] * (width // HEAD_SIZE), axis=1))
            total = jnp.sum(weights, axis=1, keepdims=True)
            mixed = jnp.dot(weights.astype(jnp.bfloat16), values,
                            preferred_element_type=jnp.float32)
            peak = jnp.maximum(jnp.max(jnp.abs(mixed), axis=1, keepdims=True), TINY)
            steps = jnp.round(mixed * (STEPS / peak)).astype(jnp.int32)
            o_send[slot, pl.ds(begin, CHUNK), h] = steps.astype(SENT).reshape(
                CHUNK, lines, HEAD_SIZE)
            peak = peak * (1.0 / (STEPS * total))
            facts = jnp.where(is_level, top + lanes(jnp.log2(total)), lanes(peak))
            l_cols[pl.ds(begin, CHUNK), h] = facts.reshape(CHUNK, lines, HEAD_SIZE)

        def returned(h):
            @pl.loop(0, CHUNK)
            def _(offset):
                @pl.when(me != begin + offset)
                def _():
                    head_copy(begin + offset, slot, h).start()

        ready = scored(0)
        for h in range(half):
            finished(h, *ready)
            if h + 1 < half:
                scores, top = scored(h + 1)
                held[:, :width] = scores
                held_top[...] = top
            if slot == 1 and h == 0:
                @pl.when(turn == 0)
                def _():
                    query_span(0, 1, CHUNK).wait_recv()
                    for i in range(CHUNK):
                        relay_copy(i).start()
            returned(h)
            if h + 1 < half:
                ready = (held[:, :width], held_top[...])

        @pl.loop(0, CHUNK)
        def _(offset):
            dst = begin + offset
            turned = l_cols[dst].reshape(half * lines, HEAD_SIZE).T
            l_send[slot, dst] = turned[0:2]

            @pl.when(me != dst)
            def _():
                facts_copy(dst, slot).start()

            @pl.when(me == dst)
            def _():
                o_recv[slot, me] = o_send[slot, dst]
                l_recv[slot, me] = l_send[slot, dst]

    low, high = jnp.where(chip < 2, 0, first_end), jnp.where(chip < 2, first_end, second_end)
    row = lax.broadcasted_iota(jnp.int32, (2 * lines, HEAD_SIZE), 0)

    def suffix_values():
        pool_copies[1].wait()

        @pl.loop(0, 2 * pairs)
        def _(batch):
            p, pair = batch // pairs, batch % pairs
            wanted = pl.ds(pl.multiple_of(pair * 2 * HEAD_SIZE, 2 * HEAD_SIZE), 2 * HEAD_SIZE)
            weights = suf_w[batch]
            mixed = None
            for rank in range(most):
                s = order[p * most + rank]
                mine = jnp.where(row % most == rank, 1.0, 0.0).astype(jnp.bfloat16)
                mine = jnp.concatenate([mine] * (span // HEAD_SIZE), axis=1)
                part = jnp.dot(weights * mine, gathered(pool_v, s, wanted),
                               preferred_element_type=jnp.float32)
                mixed = part if mixed is None else mixed + part
            level, inverse = standing(suf_s[batch, 0:1]), standing(suf_s[batch, 1:2])
            for i in range(2):
                mine = slice(i * lines, (i + 1) * lines)
                suf_o[p, pair * 2 + i] = (
                    mixed[mine, i * HEAD_SIZE:(i + 1) * HEAD_SIZE] * inverse[mine])
                suf_l[p, pair * 2 + i] = level[mine]

    @pl.loop(0, 2)
    def _(step):
        @pl.when(chip == 1)
        def _():
            prompt_turn(1, step, first_end, second_end, 1)

        prompt_turn(0, jnp.where(chip == 1, 1 - step, step), low, high, 0)

        @pl.when((chip == 1) & (step == 1))
        def _():
            suffix_half(1)

        @pl.when(step == jnp.where(chip == 1, 1, 0))
        def _():
            suffix_values()

    def merge(p):
        for d in range(2):
            arrived, levels = [], []
            if p == 1:
                @pl.when(me != 2 + d)
                def _():
                    wait_back(1, 2, d, 1)

            inside = (me // CHUNK == p) & (core == d)

            @pl.when(inside)
            def _():
                wait_back(0, p, d, 1)

            @pl.when(jnp.logical_not(inside))
            def _():
                wait_back(0, p, d, 2)

            for c, slot in HOLDERS[p]:
                sender = 2 * c + d
                levels.append((standing(l_recv[slot, sender, 0:1]), standing(l_recv[slot, sender, 1:2])))
                arrived.append((slot, sender))
            for hh in range(half):
                h = d * half + hh
                mine = slice(hh * lines, (hh + 1) * lines)
                parts = [(level[mine], o_recv[slot, sender, hh].astype(jnp.int32).astype(jnp.float32)
                          * step[mine])
                         for (level, step), (slot, sender) in zip(levels, arrived)]
                parts.append((suf_l[p, h], suf_o[p, h]))
                joint = functools.reduce(jnp.maximum, [level for level, _ in parts])
                factors = [jnp.exp2(level - joint) for level, _ in parts]
                total = functools.reduce(jnp.add, factors)
                blend = functools.reduce(jnp.add, [f * o for f, (_, o) in zip(factors, parts)])
                blend = blend / total
                for g in range(group):
                    first = (h * group + g) * HEAD_SIZE
                    merged[p * most:(p + 1) * most, first:first + HEAD_SIZE] = (
                        blend[g * most:(g + 1) * most])

    @pl.when(me < CHUNK)
    def _():
        merge(1)

    merge(0)

    @pl.when(me >= CHUNK)
    def _():
        merge(1)

    for s in range(rows):
        out_ref[s:s + 1, :] = merged[pl.ds(places[s], 1), :]

    for i in range(2):
        both_heads(i).wait_send()

    @pl.when(chip < 2)
    def _():
        query_span(0, 0, devices - 1).wait_send()

    @pl.when(chip >= 2)
    def _():
        query_span(0, 0, devices - 3).wait_send()

    @pl.when(chip == 1)
    def _():
        query_span(1, 0, 1).wait_send()
        pltpu.make_async_remote_copy(
            src_ref=q_all.at[0, pl.ds(CHUNK, CHUNK)], dst_ref=q_all.at[0, pl.ds(CHUNK, CHUNK)],
            send_sem=relay_sem.at[0], recv_sem=qr_sem.at[0, 1],
            device_id={"kv": core}, device_id_type=pl.DeviceIdType.MESH).wait_send()
        for span_copy in back_spans(1, 2, 0, devices - 1):
            span_copy.wait_send()

    @pl.when(chip != 1)
    def _():
        query_span(1, 0, 2).wait_send()

    for span_copy in back_spans(0, 0, 0, devices - 1):
        span_copy.wait_send()


def fused(
    queries,
    prompt_of,
    prompt_len,
    suffix_len,
    page_table,
    prompt_keys,
    shared_prompt_values,
    suffix_pool_keys,
    suffix_pool_values,
):
    rows, width = queries.shape
    most = rows // 2
    positions, depth = prompt_keys.shape
    heads = depth // HEAD_SIZE
    half = heads // 2
    group = width // depth
    lines = group * most
    span = page_table.shape[1] * suffix_pool_keys.shape[1]
    devices = lax.axis_size("kv")
    f32, bf16 = jnp.float32, jnp.bfloat16
    vmem, dma = pltpu.VMEM, pltpu.SemaphoreType.DMA
    return pl.pallas_call(
        attend,
        out_shape=pltpu.VMEM((rows, width), f32),
        in_specs=[pl.BlockSpec(memory_space=pl.ANY)] * 9,
        out_specs=pl.BlockSpec(memory_space=pltpu.VMEM),
        scratch_shapes=[
            pltpu.SMEM(prompt_of.shape[:1], jnp.int32),
            pltpu.SMEM(prompt_len.shape, jnp.int32),
            pltpu.SMEM(suffix_len.shape, jnp.int32),
            pltpu.SMEM(page_table.shape[::-1], jnp.int32),
            vmem((rows, width), bf16),
            pltpu.SMEM((rows,), jnp.int32),
            pltpu.SMEM((rows,), jnp.int32),
            vmem((2, heads, lines, HEAD_SIZE), f32),
            vmem((2, heads, lines, HEAD_SIZE), bf16),
            vmem((2, devices, half, lines, HEAD_SIZE), bf16),
            vmem((2, half, positions, HEAD_SIZE), bf16),
            vmem((2, half, positions, HEAD_SIZE), bf16),
            vmem(suffix_pool_keys.shape, bf16),
            vmem(suffix_pool_values.shape, bf16),
            vmem((2, devices, half, lines, HEAD_SIZE), SENT),
            vmem((2, devices, 2, HEAD_SIZE), f32),
            vmem((2, devices, half, lines, HEAD_SIZE), SENT),
            vmem((2, devices, 2, HEAD_SIZE), f32),
            vmem((devices, half, lines, HEAD_SIZE), f32),
            vmem((heads, 2 * lines, span), bf16),
            vmem((heads, 2, HEAD_SIZE), f32),
            vmem((2, heads, lines, HEAD_SIZE), f32),
            vmem((2, heads, lines, HEAD_SIZE), f32),
            vmem((rows, width), f32),
            dma((5,)),
            dma((2,)),
            dma((2,)),
            dma((2,)),
            dma((2,)),
            dma((2,)),
            dma((2, 2)),
            dma((2,)),
            dma((3, 2)),
            dma((2,)),
            dma((3, 2)),
            dma((1,)),
            pltpu.SemaphoreType.REGULAR((devices // 2,)),
            vmem((CHUNK * lines, 2 * positions), f32),
            vmem((CHUNK * lines, HEAD_SIZE), f32),
        ],
        compiler_params=pltpu.CompilerParams(
            collective_id=0, has_side_effects=True, vmem_limit_bytes=48 * 1024 * 1024
        ),
    )(
        *(pltpu.with_memory_space_constraint(array, pltpu.HBM) for array in (
            prompt_of.reshape(-1), prompt_len, suffix_len, page_table.T,
            queries, prompt_keys, shared_prompt_values, suffix_pool_keys, suffix_pool_values))
    )


def fits(mesh):
    return mesh.shape["kv"] == 8 and mesh.shape["sub"] == 1


def solution(mesh):
    body = fused if fits(mesh) else shards
    placed = (
        P(("grp", "kv"), "hd"),
        P("grp", None),
        P("grp"),
        P(("grp", "kv")),
        P(("grp", "kv"), "sub"),
        P(("grp", "kv", "sub"), "hd"),
        P(("grp", "kv", "sub"), "hd"),
        P(("grp", "kv", "sub"), None, "hd"),
        P(("grp", "kv", "sub"), None, "hd"),
    )
    return jax.shard_map(
        body, mesh=mesh, in_specs=placed, out_specs=P(("grp", "kv"), "hd"), check_vma=False
    )
```
